32 devices in a mesh: rep: 4 (over x, y), dp: 8 (over z, core).
Axes of the slice: x: 2, y: 2, z: 4, core: 2. Of those that a mesh axis runs over, the one named last changes fastest.
Arguments:
- x: bfloat16 [32, 2048, 640], P(('rep', 'dp')), parts along dimension 0
- dy: bfloat16 [32, 2048, 640], P(('rep', 'dp')), parts along dimension 0
- w_gate: bfloat16 [2, 640, 2560], replicated
- w_up: bfloat16 [2, 640, 2560], replicated
- w_down: bfloat16 [2, 2560, 640], replicated
- m_w_gate: float32 [2, 640, 2560], P(None, 'dp')
- m_w_up: float32 [2, 640, 2560], P(None, 'dp')
- m_w_down: float32 [2, 2560, 640], P(None, 'dp')
- v_w_gate: float32 [2, 640, 2560], P(None, 'dp')
- v_w_up: float32 [2, 640, 2560], P(None, 'dp')
- v_w_down: float32 [2, 2560, 640], P(None, 'dp')
Outputs:
- output 1: bfloat16 [8, 640, 2560], P('rep'), parts along dimension 0
- output 2: bfloat16 [8, 640, 2560], P('rep'), parts along dimension 0
- output 3: bfloat16 [8, 2560, 640], P('rep'), parts along dimension 0
- output 4: float32 [8, 640, 2560], P('rep', 'dp'), parts along dimension 0
- output 5: float32 [8, 640, 2560], P('rep', 'dp'), parts along dimension 0
- output 6: float32 [8, 2560, 640], P('rep', 'dp'), parts along dimension 0
- output 7: float32 [8, 640, 2560], P('rep', 'dp'), parts along dimension 0
- output 8: float32 [8, 640, 2560], P('rep', 'dp'), parts along dimension 0
- output 9: float32 [8, 2560, 640], P('rep', 'dp'), parts along dimension 0
There are 4 independent parts. The reference program is written for one: setup_inputs(seed, part) draws one part's arguments, and reference() takes and returns one part's arrays. A program takes and returns all parts, laid end to end along the dimension named above; an argument that names none is the same for every part.
All inputs are finite; a program needn't handle non-finite values.
Results may differ from the reference program's by a relative error of at most 0.022.
Values are sent between devices in bfloat16 or wider.
A program may use at most 2 GiB of HBM per device.

```python
import jax
import jax.numpy as jnp
from jax import lax

SEQUENCES = 8
TOKENS = 2048
D = 640
FF = 2560
LAYERS = 2
NAMES = ("w_gate", "w_up", "w_down")
SHAPES = {"w_gate": (LAYERS, D, FF), "w_up": (LAYERS, D, FF), "w_down": (LAYERS, FF, D)}


def bump(key, n, height):
    away = (jnp.arange(n, dtype=jnp.int32) - jax.random.randint(key, (), 0, n, jnp.int32)) % n
    return jnp.where(away < n // 8, height, 1.0)


def together(key, own, strength):
    shared = jax.random.normal(key, own.shape[1:], jnp.float32)
    return (own + strength * shared) * lax.rsqrt(1 + strength * strength)


def setup_inputs(seed: int = 0, part: int = 0) -> dict:
    kx, kdy, ka, kb, kz, kf, kh, kl, *keys = jax.random.split(jax.random.key(seed), 8 + 3 * len(NAMES))
    kx, kdy, ka, kb = (jax.random.fold_in(k, part) for k in (kx, kdy, ka, kb))
    kw, km, kv = (keys[i::3] for i in range(3))
    shape = (SEQUENCES, TOKENS, D)
    much_x, much_dy = jax.random.uniform(kz, (2,), jnp.float32, 0.0, 1.0)
    loud = 2.0 ** jax.random.uniform(jax.random.fold_in(kz, 1), (), jnp.float32, -1.0, 2.0)
    layers = 2.0 ** jax.random.uniform(kl, (LAYERS, 1, 1), jnp.float32, -1.0, 1.0)
    x = together(ka, jax.random.normal(kx, shape, jnp.float32), much_x) * bump(kf, D, 4.0)
    dy = together(kb, jax.random.normal(kdy, shape, jnp.float32), much_dy)
    drawn = {"x": x.astype(jnp.bfloat16), "dy": (loud * dy * (SEQUENCES * TOKENS) ** -0.5).astype(jnp.bfloat16)}
    for key, name in zip(kw, NAMES, strict=True):
        w = jax.random.normal(key, SHAPES[name], jnp.float32) * SHAPES[name][1] ** -0.5
        drawn[name] = (w * {"w_gate": 1.0, "w_up": bump(kh, FF, 4.0), "w_down": layers}[name]).astype(jnp.bfloat16)
    for key, name in zip(km, NAMES, strict=True):
        drawn[f"m_{name}"] = 0.1 * jax.random.normal(key, SHAPES[name], jnp.float32)
    for key, name in zip(kv, NAMES, strict=True):
        drawn[f"v_{name}"] = jax.random.uniform(key, SHAPES[name], jnp.float32, 0.005, 0.015)
    return drawn


def matmul(a, w):
    return jnp.dot(a, w, preferred_element_type=jnp.float32).astype(jnp.bfloat16)


def normed(h):
    wide = h.astype(jnp.float32)
    scale = lax.rsqrt(jnp.mean(wide**2, -1, keepdims=True) + 1e-6)
    return (wide * scale).astype(jnp.bfloat16)


def layer(h, w):
    a = normed(h)
    gate = jnp.dot(a, w["w_gate"], preferred_element_type=jnp.float32)
    up = jnp.dot(a, w["w_up"], preferred_element_type=jnp.float32)
    return h + matmul((jax.nn.silu(gate) * up).astype(jnp.bfloat16), w["w_down"])


def adamw(w, m, v, g):
    m = 0.9 * m + 0.1 * g
    v = 0.95 * v + 0.05 * g * g
    step = m * lax.rsqrt(v + 1e-8) + 0.1 * w
    return (w - 0.02 * step).astype(jnp.bfloat16), m, v


def stack(weights, h):
    return lax.scan(lambda h, w: (layer(h, w), None), h, weights)[0]


def reference(x, dy, w_gate, w_up, w_down, m_w_gate, m_w_up, m_w_down, v_w_gate, v_w_up, v_w_down):
    weights = dict(zip(NAMES, (w_gate, w_up, w_down), strict=True))

    def take(so_far, sequence):
        h, by_y = sequence
        _, back = jax.vjp(lambda w: stack(w, h), weights)
        return jax.tree.map(lambda total, term: total + term.astype(jnp.float32), so_far, back(by_y)[0]), None

    none_yet = {name: jnp.zeros(w.shape, jnp.float32) for name, w in weights.items()}
    by_weights, _ = lax.scan(take, none_yet, (x, dy))
    gradients = [by_weights[name].astype(jnp.bfloat16).astype(jnp.float32) for name in NAMES]
    new = [
        adamw(w.astype(jnp.float32), m, v, g)
        for w, m, v, g in zip((w_gate, w_up, w_down), (m_w_gate, m_w_up, m_w_down), (v_w_gate, v_w_up, v_w_down), gradients, strict=True)
    ]
    return tuple(one[which] for which in range(3) for one in new)
```

```python
import jax
import jax.numpy as jnp
from jax import lax
from jax.sharding import PartitionSpec as P

NAMES = ("w_gate", "w_up", "w_down")


def normed(h):
    wide = h.astype(jnp.float32)
    scale = lax.rsqrt(jnp.mean(wide**2, -1, keepdims=True) + 1e-6)
    return (wide * scale).astype(jnp.bfloat16)


def matmul(a, w):
    return jnp.dot(a, w, preferred_element_type=jnp.float32).astype(jnp.bfloat16)


def layer(h, w):
    a = normed(h)
    gate = jnp.dot(a, w["w_gate"], preferred_element_type=jnp.float32)
    up = jnp.dot(a, w["w_up"], preferred_element_type=jnp.float32)
    return h + matmul((jax.nn.silu(gate) * up).astype(jnp.bfloat16), w["w_down"])


def adamw(w, m, v, g):
    m = 0.9 * m + 0.1 * g
    v = 0.95 * v + 0.05 * g * g
    step = m * lax.rsqrt(v + 1e-8) + 0.1 * w
    return (w - 0.02 * step).astype(jnp.bfloat16), m, v


def solution(mesh):
    n = mesh.shape["dp"]

    def step(x, dy, *arrays):
        weights, m, v = (arrays[i : i + 3] for i in (0, 3, 6))
        h, by_y = x[0], dy[0]
        layers = weights[0].shape[0]
        me = lax.axis_index("dp")
        backs = []
        for number in range(layers):
            h, back = jax.vjp(layer, h, {name: w[number] for name, w in zip(NAMES, weights)})
            backs.append(back)
        new = {}
        for number in reversed(range(layers)):
            by_y, by_w = backs[number](by_y)
            for k in (2, 0, 1):
                g = lax.psum_scatter(by_w[NAMES[k]], "dp", scatter_dimension=0, tiled=True)
                g = g.astype(jnp.float32)
                rows = g.shape[0]
                w = lax.dynamic_slice_in_dim(weights[k][number], me * rows, rows, 0)
                one, m1, v1 = adamw(w.astype(jnp.float32), m[k][number], v[k][number], g)
                new[k, number] = (lax.all_gather(one, "dp", axis=0, tiled=True), m1, v1)
        return tuple(jnp.stack([new[k, number][which] for number in range(layers)]) for which in range(3) for k in range(3))

    whole = P(None, None, None)
    rows = P(None, "dp", None)
    seq = P(("rep", "dp"), None, None)
    return jax.shard_map(
        step,
        mesh=mesh,
        in_specs=(seq, seq) + (whole,) * 3 + (rows,) * 6,
        out_specs=(P("rep", None, None),) * 3 + (P("rep", "dp", None),) * 6,
        check_vma=False,
    )
```

```python
import functools

import jax
import jax.numpy as jnp
from jax import lax
from jax.experimental import pallas as pl
from jax.experimental.pallas import tpu as pltpu
from jax.sharding import PartitionSpec as P

MESH = pl.DeviceIdType.MESH
BF = jnp.bfloat16
F32 = jnp.float32
T, D, FF = 2048, 640, 2560
C = 256
S = 128
NL = 10
NG = 20
TILE = 512
EPS = 1e-6
OWN = 4
SCHEDULE = (
    ("partner", 1), ("sum", 0, 3, 1), ("sum", 0, 2, 1), ("sum", 0, 1, 1), ("sum", 1, 3, 4), ("sum", 1, 2, 4), ("sum", 2, 3, 7),
    ("final", 1, 7), ("final", 0, 10), ("sent", 10),
    ("gather", 2, 1, 10), ("gather", 1, 0, 14), ("gather", 3, 1, 13), ("gather", 2, 0, 17), ("gather", 3, 0, 20), ("gather", 3, 2, 12),
)
LAST = max((3 + one[-1]) // 4 for one in SCHEDULE)


def chunk_of(i):
    pair, t = i % 2, i // 2
    low = t <= 2
    z1, s1 = jnp.where(low, pair, 3 - pair), jnp.where(low, t, 4 - t)
    z2, s2 = jnp.where(low, 3 - pair, pair), jnp.where(low, 4 - t, t)
    return t, z1, s1, z2, s2


def strips_of(i):
    _, z1, s1, z2, s2 = chunk_of(i)
    return pl.multiple_of(640 * z1 + S * s1, S), pl.multiple_of(640 * z2 + S * s2, S)


def down_piece(i, c, k):
    t, z1, s1, z2, s2 = chunk_of(i)
    mid = t == 2
    dest = jnp.where(mid, z1 if k == 0 else z2, jnp.where(c == 0, z1, z2))
    s = jnp.where(c == 0, s1, s2)
    off = jnp.where(mid, jnp.where(c == 0, 256, 0), 64 * (2 * s + k - 5 * c))
    return dest, pl.multiple_of(off, 64)


def norm_of(h):
    wide = h.astype(F32)
    scale = lax.rsqrt(jnp.mean(wide * wide, -1, keepdims=True) + EPS)
    return wide, scale


def dot(a, b):
    return jnp.dot(a, b, preferred_element_type=F32)


def dot_t(a, b):
    return lax.dot_general(a, b, (((1,), (1,)), ((), ())), preferred_element_type=F32)


def adamw(w, m, v, g):
    m = 0.9 * m + 0.1 * g
    v = 0.95 * v + 0.05 * g * g
    step = m * lax.rsqrt(v + 1e-8) + 0.1 * w
    return (w - 0.02 * step).astype(BF), m, v


def kernel(
    x_h, dy_h, wg_h, wu_h, wd_h, mg_h, mu_h, md_h, vg_h, vu_h, vd_h,
    nwg, nwd, omg, omu, omd, ovg, ovu, ovd,
    H, A, AT, Y, YT, ACC, HID, DG, DU, WG, WU, WD, own_g, own_d, p_g, p_d, r_g, r_d,
    st_mg, st_vg, st_wg, st_md, st_vd, st_wd,
    sem_in, sem_w, sem_ld, sem_st, sem_send, sem_loc, sem_own, sem_pg, sem_pd, sem_rg, sem_rd, sem_ag, sem_ad, sem_pa,
):
    rep, dp = lax.axis_index("rep"), lax.axis_index("dp")
    z, c = dp // 2, dp % 2
    is_end = (z == 0) | (z == 3)
    is_mid = (z == 1) | (z == 2)

    def to(dz, flip=False):
        return (rep, (z + dz) * 2 + ((1 - c) if flip else c))

    barrier = pltpu.get_barrier_semaphore()
    pl.semaphore_signal(barrier, inc=1, device_id=to(0, True), device_id_type=MESH)

    @pl.when(z > 0)
    def _():
        pl.semaphore_signal(barrier, inc=1, device_id=to(-1), device_id_type=MESH)

    @pl.when(z < 3)
    def _():
        pl.semaphore_signal(barrier, inc=1, device_id=to(1), device_id_type=MESH)

    def w_copies(n):
        layer = jnp.where((n >= 10) & (n < 20), 1, 0)
        f1, f2 = strips_of(n % NL)
        slot = n % 2
        out = []
        for k, f in enumerate((f1, f2)):
            out.append(functools.partial(pltpu.make_async_copy, wg_h.at[layer, :, pl.ds(f, S)], WG.at[slot, :, pl.ds(S * k, S)], sem_w.at[slot, k]))
            out.append(functools.partial(pltpu.make_async_copy, wu_h.at[layer, :, pl.ds(f, S)], WU.at[slot, :, pl.ds(S * k, S)], sem_w.at[slot, 2 + k]))
            out.append(functools.partial(pltpu.make_async_copy, wd_h.at[layer, pl.ds(f, S), :], WD.at[slot, pl.ds(S * k, S), :], sem_w.at[slot, 4 + k]))
        return out

    def w_start(n):
        for one in w_copies(n):
            one().start()

    def w_wait(n):
        for one in w_copies(n):
            one().wait()

    def st_copies(g):
        slot = g % 2
        layer = 1 - g // NL
        i = g % NL
        f = strips_of(i)
        loads, stores = [], []
        for q, (m_h, v_h, w_h, om, ov) in enumerate(((mg_h, vg_h, wg_h, omg, ovg), (mu_h, vu_h, wu_h, omu, ovu))):
            for k in range(2):
                at = pl.ds(f[k], S)
                j = 2 * q + k
                loads.append(functools.partial(pltpu.make_async_copy, m_h.at[layer, :, at], st_mg.at[slot, j], sem_ld.at[slot, 0, j]))
                loads.append(functools.partial(pltpu.make_async_copy, v_h.at[layer, :, at], st_vg.at[slot, j], sem_ld.at[slot, 1, j]))
                rows = pl.ds(pl.multiple_of(80 * dp, 80), 80)
                loads.append(functools.partial(pltpu.make_async_copy, w_h.at[layer, rows, at], st_wg.at[slot, j], sem_ld.at[slot, 2, j]))
                stores.append(functools.partial(pltpu.make_async_copy, st_mg.at[slot, j], om.at[layer, :, at], sem_st.at[slot, 0, j]))
                stores.append(functools.partial(pltpu.make_async_copy, st_vg.at[slot, j], ov.at[layer, :, at], sem_st.at[slot, 1, j]))
        out = [(None, loads, stores)]
        for k in range(2):
            dest, off = down_piece(i, c, k)
            at = pl.ds(off, 64)
            rows = pl.ds(pl.multiple_of(320 * dp + off, 64), 64)
            loads = [
                functools.partial(pltpu.make_async_copy, md_h.at[layer, at], st_md.at[slot, k], sem_ld.at[slot, 0, 4 + k]),
                functools.partial(pltpu.make_async_copy, vd_h.at[layer, at], st_vd.at[slot, k], sem_ld.at[slot, 1, 4 + k]),
                functools.partial(pltpu.make_async_copy, wd_h.at[layer, rows], st_wd.at[slot, k], sem_ld.at[slot, 2, 4 + k]),
            ]
            stores = [
                functools.partial(pltpu.make_async_copy, st_md.at[slot, k], omd.at[layer, at], sem_st.at[slot, 0, 4 + k]),
                functools.partial(pltpu.make_async_copy, st_vd.at[slot, k], ovd.at[layer, at], sem_st.at[slot, 1, 4 + k]),
            ]
            out.append((dest == z, loads, stores))
        return out

    def st_do(g, which, act):
        for cond, *lists in st_copies(g):
            def go(copies=lists[which]):
                for one in copies:
                    getattr(one(), act)()
            if cond is None:
                go()
            else:
                pl.when(cond)(go)

    def rs_copy_g(g, j, dz):
        to_dest = (dz == -1) & (j == z - 1)
        slot = jnp.where(to_dest, 4, j)
        return pltpu.make_async_remote_copy(
            p_g.at[g, j], r_g.at[g, slot], sem_send.at[0], sem_rg.at[g, slot], device_id=to(dz), device_id_type=MESH)

    def rs_copy_d(g, k, dz):
        side = jnp.where(dz == 1, 0, 1)
        return pltpu.make_async_remote_copy(
            p_d.at[g, k], r_d.at[g, k, side], sem_send.at[1], sem_rd.at[g, k, side], device_id=to(dz), device_id_type=MESH)

    def wait_rg(g, slot):
        pltpu.make_async_remote_copy(
            p_g.at[g, 0], r_g.at[g, slot], sem_send.at[0], sem_rg.at[g, slot], device_id=to(0, True), device_id_type=MESH).wait_recv()

    def wait_rd(g, k, side):
        pltpu.make_async_remote_copy(
            p_d.at[g, k], r_d.at[g, k, side], sem_send.at[1], sem_rd.at[g, k, side], device_id=to(0, True), device_id_type=MESH).wait_recv()

    def ag_start_g(g, d, src, dz):
        pltpu.make_async_remote_copy(
            src, nwg.at[g, c, d], sem_send.at[2], sem_ag.at[g, d], device_id=to(dz), device_id_type=MESH).start()

    def ag_start_d(g, k, src, dz):
        pltpu.make_async_remote_copy(
            src, nwd.at[g, c, k], sem_send.at[3], sem_ad.at[g, k], device_id=to(dz), device_id_type=MESH).start()

    def partner_start_g(g, d, src):
        pltpu.make_async_remote_copy(
            src, nwg.at[g, c, d], sem_send.at[4], sem_pa.at[0], device_id=to(0, True), device_id_type=MESH).start()

    def partner_start_d(g, k, src):
        pltpu.make_async_remote_copy(
            src, nwd.at[g, c, k], sem_send.at[5], sem_pa.at[1], device_id=to(0, True), device_id_type=MESH).start()

    def wait_ag(g, d):
        pltpu.make_async_remote_copy(
            nwg.at[g, c, d], nwg.at[g, c, d], sem_send.at[2], sem_ag.at[g, d], device_id=to(0, True), device_id_type=MESH).wait_recv()

    def wait_ad(g, k):
        pltpu.make_async_remote_copy(
            nwd.at[g, c, k], nwd.at[g, c, k], sem_send.at[3], sem_ad.at[g, k], device_id=to(0, True), device_id_type=MESH).wait_recv()

    def own_copies(g):
        slot = g % OWN
        return (
            functools.partial(pltpu.make_async_remote_copy,
                own_g.at[slot, 1 - c], p_g.at[g], sem_own.at[slot, 0], sem_pg.at[g], device_id=to(0, True), device_id_type=MESH),
            functools.partial(pltpu.make_async_remote_copy,
                own_d.at[slot, 1 - c], p_d.at[g], sem_own.at[slot, 1], sem_pd.at[g], device_id=to(0, True), device_id_type=MESH),
        )

    def sum_g(g, j, *slots):
        out = own_g[g % OWN, c, j].astype(F32) + p_g[g, j].astype(F32)
        for slot in slots:
            out = out + r_g[g, slot].astype(F32)
        return out.astype(BF)

    def sum_d(g, k, *sides):
        out = own_d[g % OWN, c, k].astype(F32) + p_d[g, k].astype(F32)
        for side in sides:
            out = out + r_d[g, k, side].astype(F32)
        return out.astype(BF)

    def dest_of(g, k):
        return down_piece(g % NL, c, k)[0]

    def final(g, both):
        slot = g % 2
        st_do(g, 0, "wait")
        if both:
            wait_rg(g, z)
            wait_rg(g, 4)
            total = sum_g(g, z, z, 4)
        else:
            r = jnp.where(z == 0, 4, z)
            wait_rg(g, r)
            total = sum_g(g, z, r)
        for j in range(4):
            rows, cols = slice(80 * (j // 2), 80 * (j // 2) + 80), slice(S * (j % 2), S * (j % 2) + S)
            new, m, v = adamw(st_wg[slot, j].astype(F32), st_mg[slot, j], st_vg[slot, j], total[rows, cols].astype(F32))
            p_g[g, z, rows, cols] = new
            st_mg[slot, j] = m
            st_vg[slot, j] = v
        here = p_g.at[g, z]
        if both:
            ag_start_g(g, z, here, 1)
            ag_start_g(g, z, here, -1)
        else:
            ag_start_g(g, z, here, jnp.where(z == 0, 1, -1))
        partner_start_g(g, z, here)
        pltpu.make_async_copy(here, nwg.at[g, c, z], sem_loc).start()
        for k in range(2):
            d = dest_of(g, k)

            @pl.when(d == z)
            def _():
                if both:
                    wait_rd(g, k, 0)
                    wait_rd(g, k, 1)
                    total = sum_d(g, k, 0, 1)
                else:
                    side = jnp.where(z == 0, 1, 0)
                    wait_rd(g, k, side)
                    total = sum_d(g, k, side)
                new, m, v = adamw(st_wd[slot, k].astype(F32), st_md[slot, k], st_vd[slot, k], total.astype(F32))
                p_d[g, k] = new
                st_md[slot, k] = m
                st_vd[slot, k] = v
                here = p_d.at[g, k]
                if both:
                    ag_start_d(g, k, here, 1)
                    ag_start_d(g, k, here, -1)
                else:
                    ag_start_d(g, k, here, jnp.where(z == 0, 1, -1))
                partner_start_d(g, k, here)
                pltpu.make_async_copy(here, nwd.at[g, c, k], sem_loc).start()

        st_do(g, 1, "start")

        @pl.when(g + 1 < NG)
        def _():
            @pl.when(g >= 1)
            def _():
                st_do(g - 1, 1, "wait")
            st_do(g + 1, 0, "start")

    def mirrored(rz, rd):
        plain = z == rz
        return plain | (z == 3 - rz), jnp.where(plain, rd, 3 - rd), jnp.where(plain, 1, -1), jnp.where(plain, 0, 1)

    def reduce_step(g, rz, rd):
        active, d, dz, side = mirrored(rz, rd)

        @pl.when(active)
        def _():
            if rz == 0:
                p_g[g, d] = sum_g(g, d)
            else:
                wait_rg(g, d)
                p_g[g, d] = sum_g(g, d, d)
            rs_copy_g(g, d, dz).start()
            for k in range(2):
                @pl.when(dest_of(g, k) == d)
                def _():
                    if rz == 0:
                        p_d[g, k] = sum_d(g, k)
                    else:
                        wait_rd(g, k, side)
                        p_d[g, k] = sum_d(g, k, side)
                    rs_copy_d(g, k, dz).start()

    def final_step(g, rz):
        pl.when((z == rz) | (z == 3 - rz))(lambda: final(g, rz == 1))

    def gather_step(g, rz, rd):
        active, d, dz, _ = mirrored(rz, rd)

        @pl.when(active)
        def _():
            wait_ag(g, d)
            here = nwg.at[g, c, d]
            if rz < 3:
                ag_start_g(g, d, here, dz)
            partner_start_g(g, d, here)
            for k in range(2):
                @pl.when(dest_of(g, k) == d)
                def _():
                    wait_ad(g, k)
                    here = nwd.at[g, c, k]
                    if rz < 3:
                        ag_start_d(g, k, here, dz)
                    partner_start_d(g, k, here)

    def partner_step(g):
        for one in own_copies(g):
            one().wait_recv()

    def own_sent(g):
        for one in own_copies(g):
            one().wait_send()

    steps = {"partner": partner_step, "sum": reduce_step, "final": final_step, "gather": gather_step, "sent": own_sent}

    def tick(it, s):
        todo = [((3 + o) // 4, n, step) for n, (*step, o) in enumerate(SCHEDULE) if (3 + o) % 4 == s]
        for lag, _, (name, *rest) in sorted(todo, key=lambda one: (-one[0], one[1])):
            when_chunk(it - lag, functools.partial(lambda g, name, rest: steps[name](g, *rest), name=name, rest=rest))

    def when_chunk(g, fn):
        pl.when((g >= 0) & (g < NG))(lambda: fn(g))

    x_in = pltpu.make_async_copy(x_h, H, sem_in.at[0])
    y_in = pltpu.make_async_copy(dy_h, Y, sem_in.at[1])
    x_in.start()
    y_in.start()
    w_start(0)
    st_do(0, 0, "start")
    ROWS = 256

    def norm_rows(i):
        rows = pl.ds(pl.multiple_of(i * ROWS, ROWS), ROWS)
        wide, scale = norm_of(H[rows, :])
        a = (wide * scale).astype(BF)
        A[rows, :] = a
        return rows, a

    x_in.wait()

    @pl.loop(0, T // ROWS)
    def _(i):
        rows, _ = norm_rows(i)
        ACC[rows, :] = jnp.zeros((ROWS, D), F32)

    @pl.loop(0, NL)
    def _(n):
        slot = n % 2
        w_wait(n)
        w_start(n + 1)

        @pl.loop(0, T // TILE)
        def _(i):
            rows = pl.ds(pl.multiple_of(i * TILE, TILE), TILE)
            a = A[rows, :]
            gate = dot(a, WG[slot])
            up = dot(a, WU[slot])
            hid = (gate * jax.nn.sigmoid(gate) * up).astype(BF)
            ACC[rows, :] += dot(hid, WD[slot])

    y_in.wait()

    @pl.loop(0, T // ROWS)
    def _(i):
        rows = pl.ds(pl.multiple_of(i * ROWS, ROWS), ROWS)
        H[rows, :] = (H[rows, :].astype(F32) + ACC[rows, :].astype(BF).astype(F32)).astype(BF)
        rows, a = norm_rows(i)
        AT[:, rows] = a.T
        YT[:, rows] = Y[rows, :].T
        ACC[rows, :] = jnp.zeros((ROWS, D), F32)

    pl.semaphore_wait(barrier, 1 + jnp.where(z > 0, 1, 0) + jnp.where(z < 3, 1, 0))

    def between_layers():
        @pl.loop(0, T // ROWS)
        def _(i):
            rows = pl.ds(pl.multiple_of(i * ROWS, ROWS), ROWS)
            wide, scale = norm_of(H[rows, :])
            ct = ACC[rows, :].astype(BF).astype(F32)
            by_scale = jnp.sum(ct * wide, -1, keepdims=True)
            by_h = ct * scale - wide * (by_scale * scale * scale * scale * (1.0 / D))
            y = (Y[rows, :].astype(F32) + by_h.astype(BF).astype(F32)).astype(BF)
            Y[rows, :] = y
            YT[:, rows] = y.T

        x_again = pltpu.make_async_copy(x_h, H, sem_in.at[0])
        x_again.start()
        x_again.wait()

        @pl.loop(0, T // ROWS)
        def _(i):
            rows, a = norm_rows(i)
            AT[:, rows] = a.T

    def tiles(g, first, last):
        slot = g % 2

        @pl.loop(first, last)
        def _(i):
            rows = pl.ds(pl.multiple_of(i * TILE, TILE), TILE)
            a = A[rows, :]
            gate = dot(a, WG[slot])
            up = dot(a, WU[slot])
            by_hid = dot_t(Y[rows, :], WD[slot]).astype(BF).astype(F32)
            sig = jax.nn.sigmoid(gate)
            silu = gate * sig
            HID[rows, :] = (silu * up).astype(BF)
            DU[rows, :] = (by_hid * silu).astype(BF)
            DG[rows, :] = (by_hid * up * (sig + silu * (1.0 - sig))).astype(BF)

            @pl.when(g < NL)
            def _():
                ACC[rows, :] += dot_t(DG[rows, :], WG[slot]) + dot_t(DU[rows, :], WU[slot])

    def weight_grad(g, src, q):
        slot = g % OWN
        out = dot(AT[...], src[...]).astype(BF)
        for b in range(8):
            own_g[slot, b % 2, b // 2, 80 * q : 80 * q + 80, :] = out[80 * b : 80 * b + 80, :]

    def down_grad(g):
        slot = g % OWN
        out = dot(YT[...], HID[...]).T.astype(BF)
        mid = (g % NL) // 2 == 2
        for strip in range(2):
            for half in range(2):
                core = jnp.where(mid, half, strip)
                k = jnp.where(mid, strip, half)
                row = S * strip + 64 * half
                own_d[slot, core, k] = out[row : row + 64, :]

    @pl.loop(0, NG + LAST)
    def _(g):
        here = g < NG

        @pl.when(here)
        def _():
            w_wait(g + 10)
            pl.when(g + 1 < NG)(lambda: w_start(g + 11))
            pl.when(g == NL)(between_layers)
            tiles(g, 0, 2)

        tick(g, 0)
        pl.when(here)(lambda: tiles(g, 2, 4))
        tick(g, 1)

        @pl.when(here)
        def _():
            weight_grad(g, DG, 0)
            weight_grad(g, DU, 1)
            own_copies(g)[0]().start()

        tick(g, 2)

        @pl.when(here)
        def _():
            down_grad(g)
            own_copies(g)[1]().start()

        tick(g, 3)

    st_do(NG - 2, 1, "wait")
    st_do(NG - 1, 1, "wait")

    pltpu.make_async_copy(p_d.at[pl.ds(0, 15)], nwd.at[pl.ds(0, 15), c], sem_loc).wait()

    def all_of(ref, send, recv):
        return pltpu.make_async_remote_copy(ref, ref, send, recv, device_id=to(0, True), device_id_type=MESH)

    all_of(nwg.at[:, 1 - c], sem_send.at[4], sem_pa.at[0]).wait_recv()
    all_of(nwd.at[:, 1 - c], sem_send.at[5], sem_pa.at[1]).wait_recv()

    def sent(which, ref):
        all_of(ref, sem_send.at[which], sem_pa.at[0]).wait_send()

    sent(0, r_g.at[:, pl.ds(0, 3)])
    sent(1, p_d.at[pl.ds(0, 15)])
    sent(4, nwg.at[:, c])
    sent(5, nwd.at[:, c])

    @pl.when(is_end)
    def _():
        sent(2, r_g.at[:, 0])
        sent(3, p_d.at[pl.ds(0, 5)])

    @pl.when(is_mid)
    def _():
        sent(2, r_g)
        sent(3, r_g.at[pl.ds(0, 10)])


def train(x, dy, *arrays):
    anyspace = pl.BlockSpec(memory_space=pl.ANY)
    sds = jax.ShapeDtypeStruct
    dma = pltpu.SemaphoreType.DMA
    vm = pltpu.VMEM
    outs = (
        sds((NG, 2, 4, 160, C), BF), sds((NG, 2, 2, 64, D), BF),
        sds((2, 80, FF), F32), sds((2, 80, FF), F32), sds((2, 320, D), F32),
        sds((2, 80, FF), F32), sds((2, 80, FF), F32), sds((2, 320, D), F32),
    )
    return pl.pallas_call(
        kernel,
        out_shape=outs,
        in_specs=[anyspace] * 11,
        out_specs=(anyspace,) * 8,
        scratch_shapes=[
            vm((T, D), BF), vm((T, D), BF), vm((D, T), BF), vm((T, D), BF), vm((D, T), BF), vm((T, D), F32),
            vm((T, C), BF), vm((T, C), BF), vm((T, C), BF),
            vm((2, D, C), BF), vm((2, D, C), BF), vm((2, C, D), BF),
            vm((OWN, 2, 4, 160, C), BF), vm((OWN, 2, 2, 64, D), BF),
            vm((NG, 4, 160, C), BF), vm((NG, 2, 64, D), BF), vm((NG, 5, 160, C), BF), vm((NG, 2, 2, 64, D), BF),
            vm((2, 4, 80, S), F32), vm((2, 4, 80, S), F32), vm((2, 4, 80, S), BF),
            vm((2, 2, 64, D), F32), vm((2, 2, 64, D), F32), vm((2, 2, 64, D), BF),
            dma((2,)), dma((2, 6)), dma((2, 3, 6)), dma((2, 2, 6)), dma((6,)), dma, dma((OWN, 2)), dma((NG,)), dma((NG,)),
            dma((NG, 5)), dma((NG, 2, 2)), dma((NG, 4)), dma((NG, 2)), dma((2,)),
        ],
        compiler_params=pltpu.CompilerParams(
            collective_id=0, has_side_effects=True, vmem_limit_bytes=67000000),
        name="train",
    )(x, dy, *arrays)


def place(nwg, nwd, wg, wu, wd, buf_g, buf_d, sem_g, sem_d, sem_out):
    def load(g):
        return (
            functools.partial(pltpu.make_async_copy, nwg.at[g], buf_g.at[g], sem_g.at[g]),
            functools.partial(pltpu.make_async_copy, nwd.at[g], buf_d.at[g], sem_d.at[g]),
        )

    def store(g, act):
        layer, i = 1 - g // NL, g % NL
        f = strips_of(i)

        @pl.loop(0, 8)
        def _(b):
            rows = pl.ds(pl.multiple_of(80 * b, 80), 80)
            for q, out in enumerate((wg, wu)):
                for k in range(2):
                    src = buf_g.at[g, b % 2, b // 2, pl.ds(80 * q, 80), pl.ds(S * k, S)]
                    getattr(pltpu.make_async_copy(src, out.at[layer, rows, pl.ds(f[k], S)], sem_out.at[0]), act)()

        for core in range(2):
            for k in range(2):
                dest, off = down_piece(i, core, k)
                rows = pl.ds(pl.multiple_of(640 * dest + 320 * core + off, 64), 64)
                getattr(pltpu.make_async_copy(buf_d.at[g, core, k], wd.at[layer, rows], sem_out.at[1]), act)()

    @pl.loop(0, NG)
    def _(g):
        for one in load(g):
            one().start()

    @pl.loop(0, NG)
    def _(g):
        for one in load(g):
            one().wait()
        store(g, "start")

    @pl.loop(0, NG)
    def _(g):
        store(g, "wait")


def relayout(nwg, nwd):
    anyspace = pl.BlockSpec(memory_space=pl.ANY)
    sds = jax.ShapeDtypeStruct
    dma = pltpu.SemaphoreType.DMA
    return pl.pallas_call(
        place,
        out_shape=(sds((2, D, FF), BF), sds((2, D, FF), BF), sds((2, FF, D), BF)),
        in_specs=[anyspace] * 2,
        out_specs=(anyspace,) * 3,
        scratch_shapes=[
            pltpu.VMEM((NG, 2, 4, 160, C), BF), pltpu.VMEM((NG, 2, 2, 64, D), BF), dma((NG,)), dma((NG,)), dma((2,)),
        ],
        compiler_params=pltpu.CompilerParams(vmem_limit_bytes=50000000),
        name="place",
    )(nwg, nwd)


def solution(mesh):
    def step(x, dy, *arrays):
        nwg, nwd, *moments = train(x[0], dy[0], *arrays)
        return (*relayout(nwg, nwd), *moments)

    whole = P(None, None, None)
    rows = P(None, "dp", None)
    seq = P(("rep", "dp"), None, None)
    return jax.shard_map(
        step,
        mesh=mesh,
        in_specs=(seq, seq) + (whole,) * 3 + (rows,) * 6,
        out_specs=(P("rep", None, None),) * 3 + (P("rep", "dp", None),) * 6,
        check_vma=False,
    )
```

```python
import functools

import jax
import jax.numpy as jnp
from jax import lax
from jax.experimental import pallas as pl
from jax.experimental.pallas import tpu as pltpu
from jax.sharding import PartitionSpec as P

MESH = pl.DeviceIdType.MESH
BF = jnp.bfloat16
F32 = jnp.float32
T, D, FF = 2048, 640, 2560
C = 256
S = 128
NL = 10
NG = 20
TILE = 512
EPS = 1e-6
WS = 4
OWN = 4
PARTS = 5
FIRST = 2
SCHEDULE = (
    ("partner", "g", 0, 2), ("partner", "d", 0, 1), ("partner", "g", 1, 5), ("partner", "d", 1, 7),
    ("sum", "g", 0, 3, 2), ("sum", "d", 0, 3, 3), ("sum", "g", 0, 2, 2), ("sum", "d", 0, 2, 1), ("sum", "g", 0, 1, 6), ("sum", "d", 0, 1, 3),
    ("sum", "g", 1, 3, 5), ("sum", "d", 1, 3, 9), ("sum", "g", 1, 2, 6), ("sum", "d", 1, 2, 7), ("sum", "g", 2, 3, 9), ("sum", "d", 2, 3, 11),
    ("final", "g", 1, 9), ("final", "d", 1, 11), ("final", "g", 0, 14), ("final", "d", 0, 15), ("sent", 15),
    ("gather", "g", 2, 1, 12), ("gather", "d", 2, 1, 13), ("gather", "g", 1, 0, 17), ("gather", "d", 1, 0, 17),
    ("gather", "g", 3, 1, 19), ("gather", "d", 3, 1, 23), ("gather", "g", 2, 0, 20), ("gather", "d", 2, 0, 21),
    ("gather", "g", 3, 0, 26), ("gather", "d", 3, 0, 25), ("gather", "g", 3, 2, 21), ("gather", "d", 3, 2, 17),
)
LAST = max((FIRST + one[-1]) // PARTS for one in SCHEDULE)


def chunk_of(i):
    pair, t = i % 2, i // 2
    low = t <= 2
    z1, s1 = jnp.where(low, pair, 3 - pair), jnp.where(low, t, 4 - t)
    z2, s2 = jnp.where(low, 3 - pair, pair), jnp.where(low, 4 - t, t)
    return t, z1, s1, z2, s2


def strips_of(i):
    _, z1, s1, z2, s2 = chunk_of(i)
    return pl.multiple_of(640 * z1 + S * s1, S), pl.multiple_of(640 * z2 + S * s2, S)


def down_piece(i, c, k):
    t, z1, s1, z2, s2 = chunk_of(i)
    mid = t == 2
    dest = jnp.where(mid, z1 if k == 0 else z2, jnp.where(c == 0, z1, z2))
    s = jnp.where(c == 0, s1, s2)
    off = jnp.where(mid, jnp.where(c == 0, 256, 0), 64 * (2 * s + k - 5 * c))
    return dest, pl.multiple_of(off, 64)


def norm_of(h):
    wide = h.astype(F32)
    scale = lax.rsqrt(jnp.mean(wide * wide, -1, keepdims=True) + EPS)
    return wide, scale


def dot(a, b):
    return jnp.dot(a, b, preferred_element_type=F32)


def dot_t(a, b):
    return lax.dot_general(a, b, (((1,), (1,)), ((), ())), preferred_element_type=F32)


def adamw(w, m, v, g):
    m = 0.9 * m + 0.1 * g
    v = 0.95 * v + 0.05 * g * g
    step = m * lax.rsqrt(v + 1e-8) + 0.1 * w
    return (w - 0.02 * step).astype(BF), m, v


def kernel(
    x_h, dy_h, wg_h, wu_h, wd_h, mg_h, mu_h, md_h, vg_h, vu_h, vd_h,
    nwg, nwd, omg, omu, omd, ovg, ovu, ovd, a0_h, a0t_h, h1_h,
    HS, A, AT, Y, YT, ACC, HID, DGU, WGU, WD, own_g, own_d, p_g, p_d, x_g, x_d,
    st_mg, st_vg, st_wg, st_md, st_vd, st_wd,
    sem_in, sem_w, sem_ld, sem_st, sem_send, sem_hs, sem_own, sem_pg, sem_pd, sem_rg, sem_rd, sem_ag, sem_ad, sem_pa,
):
    rep, dp = lax.axis_index("rep"), lax.axis_index("dp")
    z, c = dp // 2, dp % 2
    is_end = (z == 0) | (z == 3)
    is_mid = (z == 1) | (z == 2)

    def to(dz, flip=False):
        return (rep, (z + dz) * 2 + ((1 - c) if flip else c))

    barrier = pltpu.get_barrier_semaphore()
    pl.semaphore_signal(barrier, inc=1, device_id=to(0, True), device_id_type=MESH)

    @pl.when(z > 0)
    def _():
        pl.semaphore_signal(barrier, inc=1, device_id=to(-1), device_id_type=MESH)

    @pl.when(z < 3)
    def _():
        pl.semaphore_signal(barrier, inc=1, device_id=to(1), device_id_type=MESH)

    def w_copies(n):
        layer = jnp.where((n >= 10) & (n < 20), 1, 0)
        slot = n % WS
        out = []
        for k, f in enumerate(strips_of(n % NL)):
            out.append(functools.partial(pltpu.make_async_copy, wg_h.at[layer, :, pl.ds(f, S)], WGU.at[slot, :, pl.ds(S * k, S)], sem_w.at[slot, k]))
            out.append(functools.partial(pltpu.make_async_copy, wu_h.at[layer, :, pl.ds(f, S)], WGU.at[slot, :, pl.ds(C + S * k, S)], sem_w.at[slot, 2 + k]))
            out.append(functools.partial(pltpu.make_async_copy, wd_h.at[layer, pl.ds(f, S), :], WD.at[slot, pl.ds(S * k, S), :], sem_w.at[slot, 4 + k]))
        return out

    def w_start(n):
        for one in w_copies(n):
            one().start()

    def w_wait(n):
        for one in w_copies(n):
            one().wait()

    def st_copies(g):
        slot = g % 2
        layer = 1 - g // NL
        i = g % NL
        f = strips_of(i)
        loads, stores = [], []
        for q, (m_h, v_h, w_h, om, ov) in enumerate(((mg_h, vg_h, wg_h, omg, ovg), (mu_h, vu_h, wu_h, omu, ovu))):
            for k in range(2):
                at = pl.ds(f[k], S)
                j = 2 * q + k
                loads.append(functools.partial(pltpu.make_async_copy, m_h.at[layer, :, at], st_mg.at[slot, j], sem_ld.at[slot, 0, j]))
                loads.append(functools.partial(pltpu.make_async_copy, v_h.at[layer, :, at], st_vg.at[slot, j], sem_ld.at[slot, 1, j]))
                rows = pl.ds(pl.multiple_of(80 * dp, 80), 80)
                loads.append(functools.partial(pltpu.make_async_copy, w_h.at[layer, rows, at], st_wg.at[slot, j], sem_ld.at[slot, 2, j]))
                stores.append(functools.partial(pltpu.make_async_copy, st_mg.at[slot, j], om.at[layer, :, at], sem_st.at[slot, 0, j]))
                stores.append(functools.partial(pltpu.make_async_copy, st_vg.at[slot, j], ov.at[layer, :, at], sem_st.at[slot, 1, j]))
        out = [(None, loads, stores)]
        for k in range(2):
            dest, off = down_piece(i, c, k)
            at = pl.ds(off, 64)
            rows = pl.ds(pl.multiple_of(320 * dp + off, 64), 64)
            loads = [
                functools.partial(pltpu.make_async_copy, md_h.at[layer, at], st_md.at[slot, k], sem_ld.at[slot, 0, 4 + k]),
                functools.partial(pltpu.make_async_copy, vd_h.at[layer, at], st_vd.at[slot, k], sem_ld.at[slot, 1, 4 + k]),
                functools.partial(pltpu.make_async_copy, wd_h.at[layer, rows], st_wd.at[slot, k], sem_ld.at[slot, 2, 4 + k]),
            ]
            stores = [
                functools.partial(pltpu.make_async_copy, st_md.at[slot, k], omd.at[layer, at], sem_st.at[slot, 0, 4 + k]),
                functools.partial(pltpu.make_async_copy, st_vd.at[slot, k], ovd.at[layer, at], sem_st.at[slot, 1, 4 + k]),
            ]
            out.append((dest == z, loads, stores))
        return out

    def st_do(g, kind, which, act):
        for cond, *lists in st_copies(g):
            if (cond is None) != (kind == "g"):
                continue
            def go(copies=lists[which]):
                for one in copies:
                    getattr(one(), act)()
            if cond is None:
                go()
            else:
                pl.when(cond)(go)

    def remote(src, dst, send, recv, where):
        return pltpu.make_async_remote_copy(src, dst, send, recv, device_id=where, device_id_type=MESH)

    def rs_start_g(g, j, dz):
        to_end = (dz == -1) & (j == z - 1)

        @pl.when(to_end)
        def _():
            remote(p_g.at[g, j], x_g.at[g], sem_send.at[0], sem_rg.at[g, 4], to(-1)).start()

        @pl.when(jnp.logical_not(to_end))
        def _():
            remote(p_g.at[g, j], nwg.at[g, c, j], sem_send.at[0], sem_rg.at[g, j], to(dz)).start()

    def rs_start_d(g, k, d, dz):
        to_end = (dz == -1) & (d == z - 1)

        @pl.when(to_end)
        def _():
            remote(p_d.at[g, k], x_d.at[g // 2, k], sem_send.at[1], sem_rd.at[g, k, 1], to(-1)).start()

        @pl.when(jnp.logical_not(to_end))
        def _():
            side = jnp.where(dz == 1, 0, 1)
            remote(p_d.at[g, k], nwd.at[g, c, k], sem_send.at[1], sem_rd.at[g, k, side], to(dz)).start()

    def wait_rg(g, slot):
        remote(p_g.at[g, 0], x_g.at[g], sem_send.at[0], sem_rg.at[g, slot], to(0, True)).wait_recv()

    def wait_rd(g, k, side):
        remote(p_d.at[g, k], x_d.at[g // 2, k], sem_send.at[1], sem_rd.at[g, k, side], to(0, True)).wait_recv()

    def ag_start_g(g, d, dz):
        here = nwg.at[g, c, d]
        remote(here, here, sem_send.at[jnp.where(dz == 1, 2, 3)], sem_ag.at[g, d], to(dz)).start()

    def ag_start_d(g, k, dz):
        here = nwd.at[g, c, k]
        remote(here, here, sem_send.at[jnp.where(dz == 1, 4, 5)], sem_ad.at[g, k], to(dz)).start()

    def partner_start_g(g, d):
        here = nwg.at[g, c, d]
        remote(here, here, sem_send.at[6], sem_pa.at[0], to(0, True)).start()

    def partner_start_d(g, k):
        here = nwd.at[g, c, k]
        remote(here, here, sem_send.at[7], sem_pa.at[1], to(0, True)).start()

    def wait_ag(g, d):
        here = nwg.at[g, c, d]
        remote(here, here, sem_send.at[2], sem_ag.at[g, d], to(0, True)).wait_recv()

    def wait_ad(g, k):
        here = nwd.at[g, c, k]
        remote(here, here, sem_send.at[4], sem_ad.at[g, k], to(0, True)).wait_recv()

    def own_copies(g):
        slot = g % OWN
        return (
            functools.partial(pltpu.make_async_remote_copy,
                own_g.at[slot, 1 - c], p_g.at[g], sem_own.at[slot, 0], sem_pg.at[g], device_id=to(0, True), device_id_type=MESH),
            functools.partial(pltpu.make_async_remote_copy,
                own_d.at[slot, 1 - c], p_d.at[g], sem_own.at[slot, 1], sem_pd.at[g], device_id=to(0, True), device_id_type=MESH),
        )

    def sum_of(*terms):
        out = terms[0].astype(F32)
        for one in terms[1:]:
            out = out + one.astype(F32)
        return out.astype(BF)

    def sum_g(g, j, *more):
        return sum_of(own_g[g % OWN, c, j], p_g[g, j], *more)

    def sum_d(g, k, *more):
        return sum_of(own_d[g % OWN, c, k], p_d[g, k], *more)

    def dest_of(g, k):
        return down_piece(g % NL, c, k)[0]

    def next_moments(g, kind):
        st_do(g, kind, 1, "start")

        @pl.when(g + 1 < NG)
        def _():
            @pl.when(g >= 1)
            def _():
                st_do(g - 1, kind, 1, "wait")
            st_do(g + 1, kind, 0, "start")

    def final_g(g, rz):
        slot = g % 2
        st_do(g, "g", 0, "wait")
        if rz == 1:
            wait_rg(g, z)
            wait_rg(g, 4)
            total = sum_g(g, z, nwg[g, c, z], x_g[g])
        else:
            @pl.when(z == 0)
            def _():
                wait_rg(g, 4)
                nwg[g, c, z] = x_g[g]

            @pl.when(z == 3)
            def _():
                wait_rg(g, z)

            total = sum_g(g, z, nwg[g, c, z])
        for j in range(4):
            rows, cols = slice(80 * (j // 2), 80 * (j // 2) + 80), slice(S * (j % 2), S * (j % 2) + S)
            new, m, v = adamw(st_wg[slot, j].astype(F32), st_mg[slot, j], st_vg[slot, j], total[rows, cols].astype(F32))
            nwg[g, c, z, rows, cols] = new
            st_mg[slot, j] = m
            st_vg[slot, j] = v
        if rz == 1:
            ag_start_g(g, z, 1)
            ag_start_g(g, z, -1)
        else:
            ag_start_g(g, z, jnp.where(z == 0, 1, -1))
        partner_start_g(g, z)
        next_moments(g, "g")

    def final_d(g, rz):
        slot = g % 2
        st_do(g, "d", 0, "wait")
        for k in range(2):
            @pl.when(dest_of(g, k) == z)
            def _():
                if rz == 1:
                    wait_rd(g, k, 0)
                    wait_rd(g, k, 1)
                    total = sum_d(g, k, nwd[g, c, k], x_d[g // 2, k])
                else:
                    @pl.when(z == 0)
                    def _():
                        wait_rd(g, k, 1)
                        nwd[g, c, k] = x_d[g // 2, k]

                    @pl.when(z == 3)
                    def _():
                        wait_rd(g, k, 0)

                    total = sum_d(g, k, nwd[g, c, k])
                new, m, v = adamw(st_wd[slot, k].astype(F32), st_md[slot, k], st_vd[slot, k], total.astype(F32))
                nwd[g, c, k] = new
                st_md[slot, k] = m
                st_vd[slot, k] = v
                if rz == 1:
                    ag_start_d(g, k, 1)
                    ag_start_d(g, k, -1)
                else:
                    ag_start_d(g, k, jnp.where(z == 0, 1, -1))
                partner_start_d(g, k)

        next_moments(g, "d")

    def mirrored(rz, rd):
        plain = z == rz
        return plain | (z == 3 - rz), jnp.where(plain, rd, 3 - rd), jnp.where(plain, 1, -1), jnp.where(plain, 0, 1)

    def reduce_step(g, kind, rz, rd):
        active, d, dz, side = mirrored(rz, rd)
        if kind == "g":
            @pl.when(active)
            def _():
                if rz == 0:
                    p_g[g, d] = sum_g(g, d)
                else:
                    wait_rg(g, d)
                    p_g[g, d] = sum_g(g, d, nwg[g, c, d])
                rs_start_g(g, d, dz)
            return
        for k in range(2):
            @pl.when(active & (dest_of(g, k) == d))
            def _():
                if rz == 0:
                    p_d[g, k] = sum_d(g, k)
                else:
                    wait_rd(g, k, side)
                    p_d[g, k] = sum_d(g, k, nwd[g, c, k])
                rs_start_d(g, k, d, dz)

    def final_step(g, kind, rz):
        final = final_g if kind == "g" else final_d
        pl.when((z == rz) | (z == 3 - rz))(lambda: final(g, rz))

    def gather_step(g, kind, rz, rd):
        active, d, dz, _ = mirrored(rz, rd)
        if kind == "g":
            @pl.when(active)
            def _():
                wait_ag(g, d)
                if rz < 3:
                    ag_start_g(g, d, dz)
                partner_start_g(g, d)
            return
        for k in range(2):
            @pl.when(active & (dest_of(g, k) == d))
            def _():
                wait_ad(g, k)
                if rz < 3:
                    ag_start_d(g, k, dz)
                partner_start_d(g, k)

    def partner_step(g, kind, rz):
        one = own_copies(g)["gd".index(kind)]
        pl.when((z == rz) | (z == 3 - rz))(lambda: one().wait_recv())

    def own_sent(g):
        for one in own_copies(g):
            one().wait_send()

    steps = {"partner": partner_step, "sum": reduce_step, "final": final_step, "gather": gather_step, "sent": own_sent}

    def tick(it, s):
        todo = [((FIRST + o) // PARTS, n, step) for n, (*step, o) in enumerate(SCHEDULE) if (FIRST + o) % PARTS == s]
        for lag, _, (name, *rest) in sorted(todo, key=lambda one: (-one[0], one[1])):
            when_chunk(it - lag, functools.partial(lambda g, name, rest: steps[name](g, *rest), name=name, rest=rest))

    def when_chunk(g, fn):
        pl.when((g >= 0) & (g < NG))(lambda: fn(g))

    ROWS = 256
    NT = T // ROWS

    def tile_of(i):
        return pl.ds(pl.multiple_of(i * ROWS, ROWS), ROWS)

    def tile_in(src, i):
        return pltpu.make_async_copy(src.at[tile_of(i)], A.at[tile_of(i)], sem_in.at[i])

    def tiles_in(src):
        @pl.loop(0, NT)
        def _(i):
            tile_in(src, i).start()

    y_in = pltpu.make_async_copy(dy_h, Y, sem_in.at[NT])
    tiles_in(x_h)
    w_start(0)
    w_start(1)
    y_in.start()
    st_do(0, "g", 0, "start")
    st_do(0, "d", 0, "start")

    @pl.loop(0, NT)
    def _(i):
        tile_in(x_h, i).wait()
        rows = tile_of(i)
        wide, scale = norm_of(A[rows, :])
        A[rows, :] = (wide * scale).astype(BF)
        ACC[rows, :] = jnp.zeros((ROWS, D), F32)

    y_in.wait()
    a_out = pltpu.make_async_copy(A, a0_h, sem_in.at[NT])
    at_out = pltpu.make_async_copy(AT, a0t_h, sem_in.at[NT + 1])
    a_out.start()

    def forward(n):
        for t in range(T // TILE):
            rows = pl.ds(t * TILE, TILE)
            a = A[rows, :]
            total = ACC[rows, :]
            for slot in ((2 * n) % WS, (2 * n + 1) % WS):
                both = dot(a, WGU[slot])
                gate, up = both[:, :C], both[:, C:]
                hid = (gate * jax.nn.sigmoid(gate) * up).astype(BF)
                total = total + dot(hid, WD[slot])
            ACC[rows, :] = total

    @pl.loop(0, NL // 2)
    def _(n):
        w_wait(2 * n)
        w_wait(2 * n + 1)
        w_start(2 * n + 2)
        w_start(2 * n + 3)
        forward(n)

        @pl.when(n < T // TILE)
        def _():
            rows = pl.ds(pl.multiple_of(n * TILE, TILE), TILE)
            AT[:, rows] = A[rows, :].T
            YT[:, rows] = Y[rows, :].T

    at_out.start()
    a_out.wait()
    tiles_in(x_h)
    at_out.wait()

    def h1_out(i):
        return pltpu.make_async_copy(HS.at[i % 2], h1_h.at[tile_of(i)], sem_hs.at[i % 2])

    @pl.loop(0, NT)
    def _(i):
        pl.when(i >= 2)(lambda: h1_out(i - 2).wait())
        tile_in(x_h, i).wait()
        rows = tile_of(i)
        h = (A[rows, :].astype(F32) + ACC[rows, :].astype(BF).astype(F32)).astype(BF)
        HS[i % 2] = h
        h1_out(i).start()
        wide, scale = norm_of(h)
        a = (wide * scale).astype(BF)
        A[rows, :] = a
        AT[:, rows] = a.T
        ACC[rows, :] = jnp.zeros((ROWS, D), F32)

    h1_out(NT - 2).wait()
    h1_out(NT - 1).wait()
    pl.semaphore_wait(barrier, 1 + jnp.where(z > 0, 1, 0) + jnp.where(z < 3, 1, 0))

    at_in = pltpu.make_async_copy(a0t_h, AT, sem_in.at[NT])

    def between_layers():
        @pl.loop(0, NT)
        def _(i):
            tile_in(h1_h, i).wait()
            rows = tile_of(i)
            wide, scale = norm_of(A[rows, :])
            ct = ACC[rows, :].astype(BF).astype(F32)
            by_scale = jnp.sum(ct * wide, -1, keepdims=True)
            by_h = ct * scale - wide * (by_scale * scale * scale * scale * (1.0 / D))
            y = (Y[rows, :].astype(F32) + by_h.astype(BF).astype(F32)).astype(BF)
            Y[rows, :] = y
            YT[:, rows] = y.T
            tile_in(a0_h, i).start()

        @pl.loop(0, NT)
        def _(i):
            tile_in(a0_h, i).wait()

        at_in.wait()

    def tiles(g, first, last):
        slot = (g + NL) % WS
        for t in range(first, last):
            rows = pl.ds(t * TILE, TILE)
            both = dot(A[rows, :], WGU[slot])
            gate, up = both[:, :C], both[:, C:]
            by_hid = dot_t(Y[rows, :], WD[slot]).astype(BF).astype(F32)
            sig = jax.nn.sigmoid(gate)
            silu = gate * sig
            HID[rows, :] = (silu * up).astype(BF)
            DGU[rows, C:] = (by_hid * silu).astype(BF)
            DGU[rows, :C] = (by_hid * up * (sig + silu * (1.0 - sig))).astype(BF)

    def input_grad(g):
        slot = (g + NL) % WS
        for t in range(T // TILE):
            rows = pl.ds(t * TILE, TILE)
            ACC[rows, :] += dot_t(DGU[rows, :], WGU[slot])

    def weight_grads(g):
        slot = g % OWN
        out = dot(AT[...], DGU[...]).astype(BF)
        for q in range(2):
            for b in range(8):
                own_g[slot, b % 2, b // 2, 80 * q : 80 * q + 80, :] = out[80 * b : 80 * b + 80, C * q : C * q + C]

    def down_grad(g):
        slot = g % OWN
        out = dot(YT[...], HID[...]).T.astype(BF)
        mid = (g % NL) // 2 == 2
        for strip in range(2):
            for half in range(2):
                core = jnp.where(mid, half, strip)
                k = jnp.where(mid, strip, half)
                row = S * strip + 64 * half
                own_d[slot, core, k] = out[row : row + 64, :]

    def part(g, s):
        if s == 0:
            w_wait(g + NL)
            pl.when(g + 2 < NG)(lambda: w_start(g + NL + 2))
            pl.when(g == NL)(between_layers)
            tiles(g, 0, 2)
        elif s == 1:
            tiles(g, 2, 4)
            pl.when(g == NL - 1)(lambda: tiles_in(h1_h))
        elif s == 2:
            weight_grads(g)
            own_copies(g)[0]().start()
            pl.when(g == NL - 1)(at_in.start)
        elif s == 3:
            down_grad(g)
            own_copies(g)[1]().start()
        else:
            pl.when(g < NL)(lambda: input_grad(g))

    @pl.loop(0, NG + LAST)
    def _(g):
        for s in range(PARTS):
            pl.when(g < NG)(functools.partial(part, g, s))
            tick(g, s)

    for kind in "gd":
        st_do(NG - 2, kind, 1, "wait")
        st_do(NG - 1, kind, 1, "wait")

    def all_of(ref, send, recv):
        return remote(ref, ref, send, recv, to(0, True))

    all_of(nwg.at[:, 1 - c], sem_send.at[6], sem_pa.at[0]).wait_recv()
    all_of(nwd.at[:, 1 - c], sem_send.at[7], sem_pa.at[1]).wait_recv()

    def sent(which, ref):
        all_of(ref, sem_send.at[which], sem_pa.at[0]).wait_send()

    sent(0, nwg.at[:, 0, pl.ds(0, 3)])
    sent(1, p_d.at[pl.ds(0, 15)])
    sent(6, nwg.at[:, c])
    sent(7, nwd.at[:, c])

    for zz in range(4):
        right, left = ((1, 0), (2, 3), (3, 2), (0, 1))[zz]

        @pl.when(z == zz)
        def _():
            if right:
                sent(2, nwg.at[:, 0, pl.ds(0, right)])
                sent(4, p_d.at[pl.ds(0, 5 * right)])
            if left:
                sent(3, nwg.at[:, 0, pl.ds(0, left)])
                sent(5, p_d.at[pl.ds(0, 5 * left)])


def train(x, dy, *arrays):
    anyspace = pl.BlockSpec(memory_space=pl.ANY)
    sds = jax.ShapeDtypeStruct
    dma = pltpu.SemaphoreType.DMA
    vm = pltpu.VMEM
    outs = (
        vm((NG, 2, 4, 160, C), BF), vm((NG, 2, 2, 64, D), BF),
        sds((2, 80, FF), F32), sds((2, 80, FF), F32), sds((2, 320, D), F32),
        sds((2, 80, FF), F32), sds((2, 80, FF), F32), sds((2, 320, D), F32),
        sds((T, D), BF), sds((D, T), BF), sds((T, D), BF),
    )
    return pl.pallas_call(
        kernel,
        out_shape=outs,
        in_specs=[anyspace] * 11,
        out_specs=(pl.BlockSpec(memory_space=pltpu.VMEM),) * 2 + (anyspace,) * 9,
        scratch_shapes=[
            vm((2, 256, D), BF), vm((T, D), BF), vm((D, T), BF), vm((T, D), BF), vm((D, T), BF), vm((T, D), F32),
            vm((T, C), BF), vm((T, 2 * C), BF), vm((WS, D, 2 * C), BF), vm((WS, C, D), BF),
            vm((OWN, 2, 4, 160, C), BF), vm((OWN, 2, 2, 64, D), BF),
            vm((NG, 4, 160, C), BF), vm((NG, 2, 64, D), BF), vm((NG, 160, C), BF), vm((NG // 2, 2, 64, D), BF),
            vm((2, 4, 80, S), F32), vm((2, 4, 80, S), F32), vm((2, 4, 80, S), BF),
            vm((2, 2, 64, D), F32), vm((2, 2, 64, D), F32), vm((2, 2, 64, D), BF),
            dma((10,)), dma((WS, 6)), dma((2, 3, 6)), dma((2, 2, 6)), dma((8,)), dma((2,)), dma((OWN, 2)), dma((NG,)), dma((NG,)),
            dma((NG, 5)), dma((NG, 2, 2)), dma((NG, 4)), dma((NG, 2)), dma((2,)),
        ],
        compiler_params=pltpu.CompilerParams(
            collective_id=0, has_side_effects=True, vmem_limit_bytes=47000000),
        name="train",
    )(x, dy, *arrays)


def place(nwg, nwd, *refs):
    moments, (wg, wu, wd), outs, (buf_mg, buf_md, sem_out, sem_m, sem_mo) = refs[:6], refs[6:9], refs[9:15], refs[15:]

    def moment(j):
        buf = buf_md.at[j // 3] if j % 3 == 2 else buf_mg.at[2 * (j // 3) + j % 3]
        return (
            functools.partial(pltpu.make_async_copy, moments[j], buf, sem_m.at[j]),
            functools.partial(pltpu.make_async_copy, buf, outs[j], sem_mo.at[j]),
        )

    def store(g, act):
        layer, i = 1 - g // NL, g % NL
        f = strips_of(i)

        @pl.loop(0, 8)
        def _(b):
            rows = pl.ds(pl.multiple_of(80 * b, 80), 80)
            for q, out in enumerate((wg, wu)):
                for k in range(2):
                    src = nwg.at[g, b % 2, b // 2, pl.ds(80 * q, 80), pl.ds(S * k, S)]
                    getattr(pltpu.make_async_copy(src, out.at[layer, rows, pl.ds(f[k], S)], sem_out.at[0]), act)()

        for core in range(2):
            for k in range(2):
                dest, off = down_piece(i, core, k)
                rows = pl.ds(pl.multiple_of(640 * dest + 320 * core + off, 64), 64)
                getattr(pltpu.make_async_copy(nwd.at[g, core, k], wd.at[layer, rows], sem_out.at[1]), act)()

    for j in range(6):
        moment(j)[0]().start()

    @pl.loop(0, NG)
    def _(g):
        store(g, "start")

    for j in range(6):
        moment(j)[0]().wait()
        moment(j)[1]().start()

    for j in range(6):
        moment(j)[1]().wait()

    @pl.loop(0, NG)
    def _(g):
        store(g, "wait")


def finish(*arrays):
    anyspace = pl.BlockSpec(memory_space=pl.ANY)
    sds = jax.ShapeDtypeStruct
    dma = pltpu.SemaphoreType.DMA
    moments = [sds(one.shape, one.dtype) for one in arrays[2:]]
    return pl.pallas_call(
        place,
        out_shape=(sds((2, D, FF), BF), sds((2, D, FF), BF), sds((2, FF, D), BF), *moments),
        in_specs=[pl.BlockSpec(memory_space=pltpu.VMEM)] * 2 + [pl.BlockSpec(memory_space=pltpu.HBM)] * 6,
        out_specs=(anyspace,) * 9,
        scratch_shapes=[
            pltpu.VMEM((4, 2, 80, FF), F32), pltpu.VMEM((2, 2, 320, D), F32),
            dma((2,)), dma((6,)), dma((6,)),
        ],
        compiler_params=pltpu.CompilerParams(vmem_limit_bytes=20000000),
        name="place",
    )(*(pltpu.with_memory_space_constraint(one, pltpu.VMEM if n < 2 else pltpu.HBM) for n, one in enumerate(arrays)))


def solution(mesh):
    def step(x, dy, *arrays):
        return finish(*train(x[0], dy[0], *arrays)[:8])

    whole = P(None, None, None)
    rows = P(None, "dp", None)
    seq = P(("rep", "dp"), None, None)
    return jax.shard_map(
        step,
        mesh=mesh,
        in_specs=(seq, seq) + (whole,) * 3 + (rows,) * 6,
        out_specs=(P("rep", None, None),) * 3 + (P("rep", "dp", None),) * 6,
        check_vma=False,
    )
```

```python
import functools

import jax
import jax.numpy as jnp
from jax import lax
from jax.experimental import pallas as pl
from jax.experimental.pallas import tpu as pltpu
from jax.sharding import PartitionSpec as P

MESH = pl.DeviceIdType.MESH
BF = jnp.bfloat16
F32 = jnp.float32
T, D, FF = 2048, 640, 2560
C = 256
S = 128
NL = 10
NG = 20
TILE = 512
EPS = 1e-6
WS = 4
OWN = 3
KEEP = 4
RING = 8
PARTS = 5
FIRST = 2
SCHEDULE = (
    ("partner", "g", 0, 2), ("partner", "d", 0, 1), ("partner", "g", 1, 5), ("partner", "d", 1, 7),
    ("sum", "g", 0, 3, 2), ("sum", "d", 0, 3, 3), ("sum", "g", 0, 2, 2), ("sum", "d", 0, 2, 1), ("sum", "g", 0, 1, 6), ("sum", "d", 0, 1, 3),
    ("sum", "g", 1, 3, 5), ("sum", "d", 1, 3, 9), ("sum", "g", 1, 2, 6), ("sum", "d", 1, 2, 7), ("sum", "g", 2, 3, 9), ("sum", "d", 2, 3, 11),
    ("final", "g", 1, 9), ("final", "d", 1, 11), ("final", "g", 0, 14), ("final", "d", 0, 15), ("sent", 12), ("sums_sent", 18),
    ("gather", "g", 2, 1, 12), ("gather", "d", 2, 1, 13), ("gather", "g", 1, 0, 17), ("gather", "d", 1, 0, 17),
    ("gather", "g", 3, 1, 19), ("gather", "d", 3, 1, 23), ("gather", "g", 2, 0, 20), ("gather", "d", 2, 0, 21),
    ("gather", "g", 3, 0, 26), ("gather", "d", 3, 0, 25), ("gather", "g", 3, 2, 21), ("gather", "d", 3, 2, 17),
)
LAST = max((FIRST + one[-1]) // PARTS for one in SCHEDULE)


def chunk_of(i):
    pair, t = i % 2, i // 2
    low = t <= 2
    z1, s1 = jnp.where(low, pair, 3 - pair), jnp.where(low, t, 4 - t)
    z2, s2 = jnp.where(low, 3 - pair, pair), jnp.where(low, 4 - t, t)
    return t, z1, s1, z2, s2


def strips_of(i):
    _, z1, s1, z2, s2 = chunk_of(i)
    return pl.multiple_of(640 * z1 + S * s1, S), pl.multiple_of(640 * z2 + S * s2, S)


def down_piece(i, c, k):
    t, z1, s1, z2, s2 = chunk_of(i)
    mid = t == 2
    dest = jnp.where(mid, z1 if k == 0 else z2, jnp.where(c == 0, z1, z2))
    s = jnp.where(c == 0, s1, s2)
    off = jnp.where(mid, jnp.where(c == 0, 256, 0), 64 * (2 * s + k - 5 * c))
    return dest, pl.multiple_of(off, 64)


def norm_of(h):
    wide = h.astype(F32)
    scale = lax.rsqrt(jnp.mean(wide * wide, -1, keepdims=True) + EPS)
    return wide, scale


def dot(a, b):
    return jnp.dot(a, b, preferred_element_type=F32)


def dot_t(a, b):
    return lax.dot_general(a, b, (((1,), (1,)), ((), ())), preferred_element_type=F32)


def adamw(w, m, v, g):
    m = 0.9 * m + 0.1 * g
    v = 0.95 * v + 0.05 * g * g
    step = m * lax.rsqrt(v + 1e-8) + 0.1 * w
    return (w - 0.02 * step).astype(BF), m, v


def kernel(
    x_h, dy_h, wg_h, wu_h, wd_h, mg_h, mu_h, md_h, vg_h, vu_h, vd_h,
    nwg, nwd, omg, omu, omd, ovg, ovu, ovd, a0_h, h1_h,
    A, AT, Y, YT, ACC, HID, DGU, WGU, WD, own_g, own_d, p_g, p_d, x_g, x_d,
    st_wg, st_wd,
    sem_in, sem_w, sem_ld, sem_send, sem_rs, sem_h, sem_own, sem_pg, sem_pd, sem_rg, sem_rd, sem_ag, sem_ad, sem_pa,
):
    rep, dp = lax.axis_index("rep"), lax.axis_index("dp")
    z, c = dp // 2, dp % 2
    is_end = (z == 0) | (z == 3)
    is_mid = (z == 1) | (z == 2)

    def to(dz, flip=False):
        return (rep, (z + dz) * 2 + ((1 - c) if flip else c))

    barrier = pltpu.get_barrier_semaphore()
    pl.semaphore_signal(barrier, inc=1, device_id=to(0, True), device_id_type=MESH)

    @pl.when(z > 0)
    def _():
        pl.semaphore_signal(barrier, inc=1, device_id=to(-1), device_id_type=MESH)

    @pl.when(z < 3)
    def _():
        pl.semaphore_signal(barrier, inc=1, device_id=to(1), device_id_type=MESH)

    def w_copies(n):
        layer = jnp.where((n >= 10) & (n < 20), 1, 0)
        slot = n % WS
        out = []
        for k, f in enumerate(strips_of(n % NL)):
            out.append(functools.partial(pltpu.make_async_copy, wg_h.at[layer, :, pl.ds(f, S)], WGU.at[slot, :, pl.ds(S * k, S)], sem_w.at[slot, k]))
            out.append(functools.partial(pltpu.make_async_copy, wu_h.at[layer, :, pl.ds(f, S)], WGU.at[slot, :, pl.ds(C + S * k, S)], sem_w.at[slot, 2 + k]))
            out.append(functools.partial(pltpu.make_async_copy, wd_h.at[layer, pl.ds(f, S), :], WD.at[slot, pl.ds(S * k, S), :], sem_w.at[slot, 4 + k]))
        return out

    def w_start(n):
        for one in w_copies(n):
            one().start()

    def w_wait(n):
        for one in w_copies(n):
            one().wait()

    def moments_in():
        return [functools.partial(pltpu.make_async_copy, src, dst, sem_ld.at[n])
                for n, (src, dst) in enumerate(((mg_h, omg), (mu_h, omu), (md_h, omd), (vg_h, ovg), (vu_h, ovu), (vd_h, ovd)))]

    def keep_weights(g):
        slot, w = g % KEEP, (g + NL) % WS
        st_wg[slot] = WGU[w, pl.ds(pl.multiple_of(80 * dp, 16), 80), :]
        mid = (g % NL) // 2 == 2
        for k in range(2):
            @pl.when(dest_of(g, k) == z)
            def _():
                row = jnp.where(mid, S * k + 64 * c, S * c + 64 * k)
                st_wd[slot, k] = WD[w, pl.ds(pl.multiple_of(row, 64), 64), :]

    def remote(src, dst, send, recv, where):
        return pltpu.make_async_remote_copy(src, dst, send, recv, device_id=where, device_id_type=MESH)

    def rs_start_g(g, j, dz):
        to_end = (dz == -1) & (j == z - 1)

        @pl.when(to_end)
        def _():
            remote(p_g.at[g % RING, j], x_g.at[g % RING], sem_rs.at[g % RING, j], sem_rg.at[g, 4], to(-1)).start()

        @pl.when(jnp.logical_not(to_end))
        def _():
            remote(p_g.at[g % RING, j], nwg.at[g, c, j], sem_rs.at[g % RING, j], sem_rg.at[g, j], to(dz)).start()

    def rs_start_d(g, k, d, dz):
        to_end = (dz == -1) & (d == z - 1)

        @pl.when(to_end)
        def _():
            remote(p_d.at[g % RING, k], x_d.at[g // 2 % (RING // 2), k], sem_rs.at[g % RING, 4 + k], sem_rd.at[g, k, 1], to(-1)).start()

        @pl.when(jnp.logical_not(to_end))
        def _():
            side = jnp.where(dz == 1, 0, 1)
            remote(p_d.at[g % RING, k], nwd.at[g, c, k], sem_rs.at[g % RING, 4 + k], sem_rd.at[g, k, side], to(dz)).start()

    def wait_rg(g, slot):
        remote(p_g.at[g % RING, 0], x_g.at[g % RING], sem_send.at[0], sem_rg.at[g, slot], to(0, True)).wait_recv()

    def wait_rd(g, k, side):
        remote(p_d.at[g % RING, k], x_d.at[g // 2 % (RING // 2), k], sem_send.at[1], sem_rd.at[g, k, side], to(0, True)).wait_recv()

    def ag_start_g(g, d, dz):
        here = nwg.at[g, c, d]
        remote(here, here, sem_send.at[jnp.where(dz == 1, 2, 3)], sem_ag.at[g, d], to(dz)).start()

    def ag_start_d(g, k, dz):
        here = nwd.at[g, c, k]
        remote(here, here, sem_send.at[jnp.where(dz == 1, 4, 5)], sem_ad.at[g, k], to(dz)).start()

    def partner_start_g(g, d):
        here = nwg.at[g, c, d]
        remote(here, here, sem_send.at[6], sem_pa.at[0], to(0, True)).start()

    def partner_start_d(g, k):
        here = nwd.at[g, c, k]
        remote(here, here, sem_send.at[7], sem_pa.at[1], to(0, True)).start()

    def wait_ag(g, d):
        here = nwg.at[g, c, d]
        remote(here, here, sem_send.at[2], sem_ag.at[g, d], to(0, True)).wait_recv()

    def wait_ad(g, k):
        here = nwd.at[g, c, k]
        remote(here, here, sem_send.at[4], sem_ad.at[g, k], to(0, True)).wait_recv()

    def own_copies(g):
        slot = g % OWN
        return (
            functools.partial(pltpu.make_async_remote_copy,
                own_g.at[slot, 1 - c], p_g.at[g % RING], sem_own.at[slot, 0], sem_pg.at[g], device_id=to(0, True), device_id_type=MESH),
            functools.partial(pltpu.make_async_remote_copy,
                own_d.at[slot, 1 - c], p_d.at[g % RING], sem_own.at[slot, 1], sem_pd.at[g], device_id=to(0, True), device_id_type=MESH),
        )

    def sum_of(*terms):
        out = terms[0].astype(F32)
        for one in terms[1:]:
            out = out + one.astype(F32)
        return out.astype(BF)

    def sum_g(g, j, *more):
        return sum_of(own_g[g % OWN, c, j], p_g[g % RING, j], *more)

    def sum_d(g, k, *more):
        return sum_of(own_d[g % OWN, c, k], p_d[g % RING, k], *more)

    def dest_of(g, k):
        return down_piece(g % NL, c, k)[0]

    def final_g(g, rz):
        slot, layer, f = g % KEEP, 1 - g // NL, strips_of(g % NL)
        if rz == 1:
            wait_rg(g, z)
            wait_rg(g, 4)
            total = sum_g(g, z, nwg[g, c, z], x_g[g % RING])
        else:
            @pl.when(z == 0)
            def _():
                wait_rg(g, 4)
                nwg[g, c, z] = x_g[g % RING]

            @pl.when(z == 3)
            def _():
                wait_rg(g, z)

            total = sum_g(g, z, nwg[g, c, z])
        for j in range(4):
            q, k = j // 2, j % 2
            rows, cols, at = slice(80 * q, 80 * q + 80), slice(S * k, S * k + S), pl.ds(f[k], S)
            om, ov = ((omg, ovg), (omu, ovu))[q]
            w = st_wg[slot, :, C * q + S * k : C * q + S * k + S].astype(F32)
            new, m, v = adamw(w, om[layer, :, at], ov[layer, :, at], total[rows, cols].astype(F32))
            nwg[g, c, z, rows, cols] = new
            om[layer, :, at] = m
            ov[layer, :, at] = v
        if rz == 1:
            ag_start_g(g, z, 1)
            ag_start_g(g, z, -1)
        else:
            ag_start_g(g, z, jnp.where(z == 0, 1, -1))
        partner_start_g(g, z)

    def final_d(g, rz):
        slot, layer = g % KEEP, 1 - g // NL
        for k in range(2):
            @pl.when(dest_of(g, k) == z)
            def _():
                if rz == 1:
                    wait_rd(g, k, 0)
                    wait_rd(g, k, 1)
                    total = sum_d(g, k, nwd[g, c, k], x_d[g // 2 % (RING // 2), k])
                else:
                    @pl.when(z == 0)
                    def _():
                        wait_rd(g, k, 1)
                        nwd[g, c, k] = x_d[g // 2 % (RING // 2), k]

                    @pl.when(z == 3)
                    def _():
                        wait_rd(g, k, 0)

                    total = sum_d(g, k, nwd[g, c, k])
                at = pl.ds(down_piece(g % NL, c, k)[1], 64)
                new, m, v = adamw(st_wd[slot, k].astype(F32), omd[layer, at, :], ovd[layer, at, :], total.astype(F32))
                nwd[g, c, k] = new
                omd[layer, at, :] = m
                ovd[layer, at, :] = v
                if rz == 1:
                    ag_start_d(g, k, 1)
                    ag_start_d(g, k, -1)
                else:
                    ag_start_d(g, k, jnp.where(z == 0, 1, -1))
                partner_start_d(g, k)

    def mirrored(rz, rd):
        plain = z == rz
        return plain | (z == 3 - rz), jnp.where(plain, rd, 3 - rd), jnp.where(plain, 1, -1), jnp.where(plain, 0, 1)

    def reduce_step(g, kind, rz, rd):
        active, d, dz, side = mirrored(rz, rd)
        if kind == "g":
            @pl.when(active)
            def _():
                if rz == 0:
                    p_g[g % RING, d] = sum_g(g, d)
                else:
                    wait_rg(g, d)
                    p_g[g % RING, d] = sum_g(g, d, nwg[g, c, d])
                rs_start_g(g, d, dz)
            return
        for k in range(2):
            @pl.when(active & (dest_of(g, k) == d))
            def _():
                if rz == 0:
                    p_d[g % RING, k] = sum_d(g, k)
                else:
                    wait_rd(g, k, side)
                    p_d[g % RING, k] = sum_d(g, k, nwd[g, c, k])
                rs_start_d(g, k, d, dz)

    def final_step(g, kind, rz):
        final = final_g if kind == "g" else final_d
        pl.when((z == rz) | (z == 3 - rz))(lambda: final(g, rz))

    def gather_step(g, kind, rz, rd):
        active, d, dz, _ = mirrored(rz, rd)
        if kind == "g":
            @pl.when(active)
            def _():
                wait_ag(g, d)
                if rz < 3:
                    ag_start_g(g, d, dz)
                partner_start_g(g, d)
            return
        for k in range(2):
            @pl.when(active & (dest_of(g, k) == d))
            def _():
                wait_ad(g, k)
                if rz < 3:
                    ag_start_d(g, k, dz)
                partner_start_d(g, k)

    def partner_step(g, kind, rz):
        one = own_copies(g)["gd".index(kind)]
        pl.when((z == rz) | (z == 3 - rz))(lambda: one().wait_recv())

    def sums_sent(g):
        slot = g % RING

        def wait(ref, at):
            remote(ref, ref, sem_rs.at[slot, at], sem_pa.at[0], to(0, True)).wait_send()

        for j in range(4):
            pl.when(z != j)(lambda j=j: wait(p_g.at[slot, j], j))
        for k in range(2):
            pl.when(dest_of(g, k) != z)(lambda k=k: wait(p_d.at[slot, k], 4 + k))

    def own_sent(g):
        for one in own_copies(g):
            one().wait_send()

    steps = {"partner": partner_step, "sum": reduce_step, "final": final_step, "gather": gather_step, "sent": own_sent, "sums_sent": sums_sent}

    def tick(it, s):
        todo = [((FIRST + o) // PARTS, n, step) for n, (*step, o) in enumerate(SCHEDULE) if (FIRST + o) % PARTS == s]
        for lag, _, (name, *rest) in sorted(todo, key=lambda one: (-one[0], one[1])):
            when_chunk(it - lag, functools.partial(lambda g, name, rest: steps[name](g, *rest), name=name, rest=rest))

    def when_chunk(g, fn):
        pl.when((g >= 0) & (g < NG))(lambda: fn(g))

    NT = T // TILE

    def tile_of(i):
        return pl.ds(pl.multiple_of(i * TILE, TILE), TILE)

    def tile_in(src, i):
        return pltpu.make_async_copy(src.at[tile_of(i)], A.at[tile_of(i)], sem_in.at[i])

    def tiles_in(src):
        @pl.loop(0, NT)
        def _(i):
            tile_in(src, i).start()

    def h_parts(i):
        rows = tile_of(i)
        return (DGU.at[rows], pl.ds(0, 512)), (HID.at[rows, pl.ds(0, 128)], pl.ds(512, 128))

    def x_again(i):
        return [functools.partial(pltpu.make_async_copy, x_h.at[tile_of(i), cols], ref, sem_h.at[0, i, k]) for k, (ref, cols) in enumerate(h_parts(i))]

    def h1_out(i):
        return [functools.partial(pltpu.make_async_copy, ref, h1_h.at[tile_of(i), cols], sem_h.at[1, i, k]) for k, (ref, cols) in enumerate(h_parts(i))]

    def each(copies, act):
        for one in copies:
            getattr(one(), act)()

    y_in = pltpu.make_async_copy(dy_h, Y, sem_in.at[NT + 1])
    tile_in(x_h, 0).start()
    w_start(0)
    w_start(1)
    for t in range(1, NT):
        tile_in(x_h, t).start()
    a_out = pltpu.make_async_copy(A, a0_h, sem_in.at[NT])

    def forward_tile(n, t):
        rows = pl.ds(t * TILE, TILE) if isinstance(t, int) else tile_of(t)
        a = A[rows, :]
        total = 0.0
        for slot in ((2 * n) % WS, (2 * n + 1) % WS):
            both = dot(a, WGU[slot])
            gate, up = both[:, :C], both[:, C:]
            hid = (gate * jax.nn.sigmoid(gate) * up).astype(BF)
            total = total + dot(hid, WD[slot])
        return rows, total

    def turn(src, dst):
        @pl.loop(0, NT)
        def _(t):
            rows = tile_of(t)
            dst[:, rows] = src[rows, :].T

    def forward_weights(n):
        w_wait(2 * n)
        w_wait(2 * n + 1)
        w_start(2 * n + 2)
        w_start(2 * n + 3)

    for t in range(NT):
        tile_in(x_h, t).wait()
        rows = pl.ds(t * TILE, TILE)
        wide, scale = norm_of(A[rows, :])
        A[rows, :] = (wide * scale).astype(BF)
        if t == 0:
            forward_weights(0)
        rows, total = forward_tile(0, t)
        ACC[rows, :] = total
    a_out.start()
    y_in.start()
    for t in range(NT):
        each(x_again(t), "start")
    each(moments_in(), "start")

    @pl.loop(1, NL // 2 - 1)
    def _(n):
        forward_weights(n)
        for t in range(NT):
            rows, total = forward_tile(n, t)
            ACC[rows, :] += total

    a_out.wait()
    forward_weights(NL // 2 - 1)
    for t in range(NT):
        each(x_again(t), "wait")
    def last_forward(t):
        rows, total = forward_tile(NL // 2 - 1, t)
        total = (ACC[rows, :] + total).astype(BF).astype(F32)
        ACC[rows, :] = jnp.zeros((TILE, D), F32)
        ha = (DGU[rows, :].astype(F32) + total[:, :512]).astype(BF)
        hb = (HID[rows, :128].astype(F32) + total[:, 512:]).astype(BF)
        DGU[rows, :] = ha
        HID[rows, :128] = hb
        ha, hb = ha.astype(F32), hb.astype(F32)
        mean = (jnp.sum(ha * ha, -1, keepdims=True) + jnp.sum(hb * hb, -1, keepdims=True)) * (1.0 / D)
        scale = lax.rsqrt(mean + EPS)
        A[rows, :512] = (ha * scale).astype(BF)
        A[rows, 512:] = (hb * scale).astype(BF)
        AT[:, rows] = A[rows, :].T
        each(h1_out(t), "start")

    @pl.loop(0, NT // 2)
    def _(i):
        last_forward(2 * i)
        last_forward(2 * i + 1)

    y_in.wait()
    turn(Y, YT)
    each(moments_in(), "wait")
    pl.semaphore_wait(barrier, 1 + jnp.where(z > 0, 1, 0) + jnp.where(z < 3, 1, 0))

    def tiles(g, first, last):
        slot = (g + NL) % WS
        for t in range(first, last):
            rows = pl.ds(t * TILE, TILE)
            both = dot(A[rows, :], WGU[slot])
            gate, up = both[:, :C], both[:, C:]
            by_hid = dot_t(Y[rows, :], WD[slot]).astype(BF).astype(F32)
            sig = jax.nn.sigmoid(gate)
            silu = gate * sig
            HID[rows, :] = (silu * up).astype(BF)
            DGU[rows, C:] = (by_hid * silu).astype(BF)
            DGU[rows, :C] = (by_hid * up * (sig + silu * (1.0 - sig))).astype(BF)

    def input_grad(g):
        slot = (g + NL) % WS
        for t in range(NT):
            rows = pl.ds(t * TILE, TILE)
            ACC[rows, :] += dot_t(DGU[rows, :], WGU[slot])

    def last_input_grad(g):
        slot = (g + NL) % WS
        for t in range(NT):
            tile_in(h1_h, t).wait()
        @pl.loop(0, NT)
        def _(t):
            rows = tile_of(t)
            ct = (ACC[rows, :] + dot_t(DGU[rows, :], WGU[slot])).astype(BF).astype(F32)
            wide, scale = norm_of(A[rows, :])
            by_scale = jnp.sum(ct * wide, -1, keepdims=True)
            by_h = ct * scale - wide * (by_scale * scale * scale * scale * (1.0 / D))
            y = (Y[rows, :].astype(F32) + by_h.astype(BF).astype(F32)).astype(BF)
            Y[rows, :] = y
            YT[:, rows] = y.T
        for t in range(NT):
            tile_in(a0_h, t).start()

    def weight_grads(g):
        slot = g % OWN
        out = dot(AT[...], DGU[...]).astype(BF)
        for q in range(2):
            for b in range(8):
                own_g[slot, b % 2, b // 2, 80 * q : 80 * q + 80, :] = out[80 * b : 80 * b + 80, C * q : C * q + C]

    def down_grad(g):
        slot = g % OWN
        out = dot(YT[...], HID[...]).T.astype(BF)
        mid = (g % NL) // 2 == 2
        for strip in range(2):
            for half in range(2):
                core = jnp.where(mid, half, strip)
                k = jnp.where(mid, strip, half)
                row = S * strip + 64 * half
                own_d[slot, core, k] = out[row : row + 64, :]

    def part(g, s):
        if s == 0:
            w_wait(g + NL)
            pl.when(g + 2 < NG)(lambda: w_start(g + NL + 2))

            @pl.when(g == 0)
            def _():
                for t in range(NT):
                    each(h1_out(t), "wait")

            @pl.when(g == NL)
            def _():
                for t in range(NT):
                    tile_in(a0_h, t).wait()
                turn(A, AT)

            keep_weights(g)
            tiles(g, 0, 2)
        elif s == 1:
            tiles(g, 2, 4)
            pl.when(g == NL - 1)(lambda: tiles_in(h1_h))
        elif s == 2:
            weight_grads(g)
            own_copies(g)[0]().start()
        elif s == 3:
            down_grad(g)
            own_copies(g)[1]().start()
        else:
            pl.when(g < NL - 1)(lambda: input_grad(g))
            pl.when(g == NL - 1)(lambda: last_input_grad(g))

    @pl.loop(0, NG + LAST)
    def _(g):
        for s in range(PARTS):
            pl.when(g < NG)(functools.partial(part, g, s))
            tick(g, s)

    def all_of(ref, send, recv):
        return remote(ref, ref, send, recv, to(0, True))

    all_of(nwg.at[:, 1 - c], sem_send.at[6], sem_pa.at[0]).wait_recv()
    all_of(nwd.at[:, 1 - c], sem_send.at[7], sem_pa.at[1]).wait_recv()

    def sent(which, ref):
        all_of(ref, sem_send.at[which], sem_pa.at[0]).wait_send()

    sent(6, nwg.at[:, c])
    sent(7, nwd.at[:, c])

    for zz in range(4):
        right, left = ((1, 0), (2, 3), (3, 2), (0, 1))[zz]

        @pl.when(z == zz)
        def _():
            if right:
                sent(2, nwg.at[:, 0, pl.ds(0, right)])
                sent(4, nwd.at[pl.ds(0, 5 * right), 0])
            if left:
                sent(3, nwg.at[:, 0, pl.ds(0, left)])
                sent(5, nwd.at[pl.ds(0, 5 * left), 0])


def train(x, dy, *arrays):
    anyspace = pl.BlockSpec(memory_space=pl.ANY)
    sds = jax.ShapeDtypeStruct
    dma = pltpu.SemaphoreType.DMA
    vm = pltpu.VMEM
    outs = (
        vm((NG, 2, 4, 160, C), BF), vm((NG, 2, 2, 64, D), BF),
        vm((2, 80, FF), F32), vm((2, 80, FF), F32), vm((2, 320, D), F32),
        vm((2, 80, FF), F32), vm((2, 80, FF), F32), vm((2, 320, D), F32),
        sds((T, D), BF), sds((T, D), BF),
    )
    return pl.pallas_call(
        kernel,
        out_shape=outs,
        in_specs=[anyspace] * 11,
        out_specs=(pl.BlockSpec(memory_space=pltpu.VMEM),) * 8 + (anyspace,) * 2,
        scratch_shapes=[
            vm((T, D), BF), vm((D, T), BF), vm((T, D), BF), vm((D, T), BF), vm((T, D), F32),
            vm((T, C), BF), vm((T, 2 * C), BF), vm((WS, D, 2 * C), BF), vm((WS, C, D), BF),
            vm((OWN, 2, 4, 160, C), BF), vm((OWN, 2, 2, 64, D), BF),
            vm((RING, 4, 160, C), BF), vm((RING, 2, 64, D), BF), vm((RING, 160, C), BF), vm((RING // 2, 2, 64, D), BF),
            vm((KEEP, 80, 2 * C), BF), vm((KEEP, 2, 64, D), BF),
            dma((10,)), dma((WS, 6)), dma((6,)), dma((8,)), dma((RING, 6)), dma((2, 4, 2)), dma((OWN, 2)), dma((NG,)), dma((NG,)),
            dma((NG, 5)), dma((NG, 2, 2)), dma((NG, 4)), dma((NG, 2)), dma((2,)),
        ],
        compiler_params=pltpu.CompilerParams(
            collective_id=0, has_side_effects=True, vmem_limit_bytes=37000000),
        name="train",
    )(x, dy, *arrays)


def place(nwg, nwd, *refs):
    moments, (wg, wu, wd), outs, (sem_out, sem_mo) = refs[:6], refs[6:9], refs[9:15], refs[15:]

    def moment(j):
        return pltpu.make_async_copy(moments[j], outs[j], sem_mo.at[j])

    def store(g, act):
        layer, i = 1 - g // NL, g % NL
        f = strips_of(i)

        @pl.loop(0, 8)
        def _(b):
            rows = pl.ds(pl.multiple_of(80 * b, 80), 80)
            for q, out in enumerate((wg, wu)):
                for k in range(2):
                    src = nwg.at[g, b % 2, b // 2, pl.ds(80 * q, 80), pl.ds(S * k, S)]
                    getattr(pltpu.make_async_copy(src, out.at[layer, rows, pl.ds(f[k], S)], sem_out.at[0]), act)()

        for core in range(2):
            for k in range(2):
                dest, off = down_piece(i, core, k)
                rows = pl.ds(pl.multiple_of(640 * dest + 320 * core + off, 64), 64)
                getattr(pltpu.make_async_copy(nwd.at[g, core, k], wd.at[layer, rows], sem_out.at[1]), act)()

    for j in range(6):
        moment(j).start()

    @pl.loop(0, NG)
    def _(g):
        store(g, "start")

    for j in range(6):
        moment(j).wait()

    @pl.loop(0, NG)
    def _(g):
        store(g, "wait")


def finish(*arrays):
    anyspace = pl.BlockSpec(memory_space=pl.ANY)
    sds = jax.ShapeDtypeStruct
    dma = pltpu.SemaphoreType.DMA
    moments = [sds(one.shape, one.dtype) for one in arrays[2:]]
    return pl.pallas_call(
        place,
        out_shape=(sds((2, D, FF), BF), sds((2, D, FF), BF), sds((2, FF, D), BF), *moments),
        in_specs=[pl.BlockSpec(memory_space=pltpu.VMEM)] * 8,
        out_specs=(anyspace,) * 9,
        scratch_shapes=[
            dma((2,)), dma((6,)),
        ],
        compiler_params=pltpu.CompilerParams(vmem_limit_bytes=2000000),
        name="place",
    )(*(pltpu.with_memory_space_constraint(one, pltpu.VMEM) for one in arrays))


def solution(mesh):
    def step(x, dy, *arrays):
        return finish(*train(x[0], dy[0], *arrays)[:8])

    whole = P(None, None, None)
    rows = P(None, "dp", None)
    seq = P(("rep", "dp"), None, None)
    return jax.shard_map(
        step,
        mesh=mesh,
        in_specs=(seq, seq) + (whole,) * 3 + (rows,) * 6,
        out_specs=(P("rep", None, None),) * 3 + (P("rep", "dp", None),) * 6,
        check_vma=False,
    )
```

```python
import functools

import jax
import jax.numpy as jnp
from jax import lax
from jax.experimental import pallas as pl
from jax.experimental.pallas import tpu as pltpu
from jax.sharding import PartitionSpec as P

MESH = pl.DeviceIdType.MESH
BF = jnp.bfloat16
F32 = jnp.float32
T, D, FF = 2048, 640, 2560
C = 256
S = 128
NL = 10
NG = 20
TILE = 512
EPS = 1e-6
WS = 4
OWN = 3
KEEP = 4
RING = 6
PARTS = 5
FIRST = 2
SCHEDULE = (
    ("partner", "g", 0, 1),
    ("partner", "g", 1, 4),
    ("partner", "d", 0, 1),
    ("partner", "d", 1, 6),
    ("sum", "g", 0, 3, 1),
    ("sum", "d", 0, 3, 2),
    ("sum", "g", 0, 2, 1),
    ("sum", "d", 0, 2, 1),
    ("sum", "g", 0, 1, 5),
    ("sum", "d", 0, 1, 3),
    ("sum", "g", 1, 3, 4),
    ("sum", "d", 1, 3, 7),
    ("sum", "g", 1, 2, 5),
    ("sum", "d", 1, 2, 6),
    ("sum", "g", 2, 3, 7),
    ("sum", "d", 2, 3, 9),
    ("final", "g", 1, 8),
    ("final", "d", 1, 9),
    ("final", "g", 0, 13),
    ("final", "d", 0, 14),
    ("gather", "g", 2, 1, 11),
    ("gather", "d", 2, 1, 12),
    ("gather", "g", 1, 0, 17),
    ("gather", "d", 1, 0, 18),
    ("gather", "g", 3, 1, 13),
    ("gather", "d", 3, 1, 23),
    ("gather", "g", 2, 0, 20),
    ("gather", "d", 2, 0, 20),
    ("gather", "g", 3, 0, 25),
    ("gather", "d", 3, 0, 29),
    ("gather", "g", 3, 2, 20),
    ("gather", "d", 3, 2, 24),
    ("sent", 12),
    ("sums_sent", 18),
)
LAST = max((FIRST + one[-1]) // PARTS for one in SCHEDULE)


def chunk_of(i):
    pair, t = i % 2, i // 2
    low = t <= 2
    z1, s1 = jnp.where(low, pair, 3 - pair), jnp.where(low, t, 4 - t)
    z2, s2 = jnp.where(low, 3 - pair, pair), jnp.where(low, 4 - t, t)
    return t, z1, s1, z2, s2


def strips_of(i):
    _, z1, s1, z2, s2 = chunk_of(i)
    return pl.multiple_of(640 * z1 + S * s1, S), pl.multiple_of(640 * z2 + S * s2, S)


def down_piece(i, c, k):
    t, z1, s1, z2, s2 = chunk_of(i)
    mid = t == 2
    dest = jnp.where(mid, z1 if k == 0 else z2, jnp.where(c == 0, z1, z2))
    s = jnp.where(c == 0, s1, s2)
    off = jnp.where(mid, jnp.where(c == 0, 256, 0), 64 * (2 * s + k - 5 * c))
    return dest, pl.multiple_of(off, 64)


def norm_of(h):
    wide = h.astype(F32)
    scale = lax.rsqrt(jnp.mean(wide * wide, -1, keepdims=True) + EPS)
    return wide, scale


def dot(a, b):
    return jnp.dot(a, b, preferred_element_type=F32)


def dot_t(a, b):
    return lax.dot_general(a, b, (((1,), (1,)), ((), ())), preferred_element_type=F32)


def adamw(w, m, v, g):
    m = 0.9 * m + 0.1 * g
    v = 0.95 * v + 0.05 * g * g
    step = m * lax.rsqrt(v + 1e-8) + 0.1 * w
    return (w - 0.02 * step).astype(BF), m, v


def kernel(
    x_h, dy_h, wg_h, wu_h, wd_h, mg_h, mu_h, md_h, vg_h, vu_h, vd_h,
    nwg, nwd, omg, omu, omd, ovg, ovu, ovd, a0_h, h1_h,
    A, AT, Y, YT, ACC, HID, DGU, WGU, WD, own_g, own_d, p_g, p_d, x_g, x_d,
    st_wg, st_wd,
    sem_in, sem_w, sem_ld, sem_send, sem_rs, sem_h, sem_own, sem_pg, sem_pd, sem_rg, sem_rd, sem_ag, sem_ad, sem_pa,
):
    rep, dp = lax.axis_index("rep"), lax.axis_index("dp")
    z, c = dp // 2, dp % 2
    is_end = (z == 0) | (z == 3)
    is_mid = (z == 1) | (z == 2)

    def to(dz, flip=False):
        return (rep, (z + dz) * 2 + ((1 - c) if flip else c))

    barrier = pltpu.get_barrier_semaphore()
    pl.semaphore_signal(barrier, inc=1, device_id=to(0, True), device_id_type=MESH)

    @pl.when(z > 0)
    def _():
        pl.semaphore_signal(barrier, inc=1, device_id=to(-1), device_id_type=MESH)

    @pl.when(z < 3)
    def _():
        pl.semaphore_signal(barrier, inc=1, device_id=to(1), device_id_type=MESH)

    def w_copies(n):
        layer = jnp.where((n >= 10) & (n < 20), 1, 0)
        slot = n % WS
        out = []
        for k, f in enumerate(strips_of(n % NL)):
            out.append(functools.partial(pltpu.make_async_copy, wg_h.at[layer, :, pl.ds(f, S)], WGU.at[slot, :, pl.ds(S * k, S)], sem_w.at[slot, k]))
            out.append(functools.partial(pltpu.make_async_copy, wu_h.at[layer, :, pl.ds(f, S)], WGU.at[slot, :, pl.ds(C + S * k, S)], sem_w.at[slot, 2 + k]))
            out.append(functools.partial(pltpu.make_async_copy, wd_h.at[layer, pl.ds(f, S), :], WD.at[slot, pl.ds(S * k, S), :], sem_w.at[slot, 4 + k]))
        return out

    def w_start(n):
        for one in w_copies(n):
            one().start()

    def w_wait(n):
        for one in w_copies(n):
            one().wait()

    def moments_in():
        return [functools.partial(pltpu.make_async_copy, src, dst, sem_ld.at[n])
                for n, (src, dst) in enumerate(((mg_h, omg), (mu_h, omu), (md_h, omd), (vg_h, ovg), (vu_h, ovu), (vd_h, ovd)))]

    def keep_weights(g):
        slot, w = g % KEEP, (g + NL) % WS
        st_wg[slot] = WGU[w, pl.ds(pl.multiple_of(80 * dp, 16), 80), :]
        mid = (g % NL) // 2 == 2
        for k in range(2):
            @pl.when(dest_of(g, k) == z)
            def _():
                row = jnp.where(mid, S * k + 64 * c, S * c + 64 * k)
                st_wd[slot, k] = WD[w, pl.ds(pl.multiple_of(row, 64), 64), :]

    def remote(src, dst, send, recv, where):
        return pltpu.make_async_remote_copy(src, dst, send, recv, device_id=where, device_id_type=MESH)

    def rs_start_g(g, j, dz):
        to_end = (dz == -1) & (j == z - 1)

        @pl.when(to_end)
        def _():
            remote(p_g.at[g % RING, j], x_g.at[g % RING], sem_rs.at[g % RING, j], sem_rg.at[g, 4], to(-1)).start()

        @pl.when(jnp.logical_not(to_end))
        def _():
            remote(p_g.at[g % RING, j], nwg.at[g, c, j], sem_rs.at[g % RING, j], sem_rg.at[g, j], to(dz)).start()

    def rs_start_d(g, k, d, dz):
        to_end = (dz == -1) & (d == z - 1)

        @pl.when(to_end)
        def _():
            remote(p_d.at[g % RING, k], x_d.at[g // 2 % (RING // 2), k], sem_rs.at[g % RING, 4 + k], sem_rd.at[g, k, 1], to(-1)).start()

        @pl.when(jnp.logical_not(to_end))
        def _():
            side = jnp.where(dz == 1, 0, 1)
            remote(p_d.at[g % RING, k], nwd.at[g, c, k], sem_rs.at[g % RING, 4 + k], sem_rd.at[g, k, side], to(dz)).start()

    def wait_rg(g, slot):
        remote(p_g.at[g % RING, 0], x_g.at[g % RING], sem_send.at[0], sem_rg.at[g, slot], to(0, True)).wait_recv()

    def wait_rd(g, k, side):
        remote(p_d.at[g % RING, k], x_d.at[g // 2 % (RING // 2), k], sem_send.at[1], sem_rd.at[g, k, side], to(0, True)).wait_recv()

    def ag_start_g(g, d, dz):
        here = nwg.at[g, c, d]
        remote(here, here, sem_send.at[jnp.where(dz == 1, 2, 3)], sem_ag.at[g, d], to(dz)).start()

    def ag_start_d(g, k, dz):
        here = nwd.at[g, c, k]
        remote(here, here, sem_send.at[jnp.where(dz == 1, 4, 5)], sem_ad.at[g, k], to(dz)).start()

    def partner_start_g(g, d):
        here = nwg.at[g, c, d]
        remote(here, here, sem_send.at[6], sem_pa.at[0], to(0, True)).start()

    def partner_start_d(g, k):
        here = nwd.at[g, c, k]
        remote(here, here, sem_send.at[7], sem_pa.at[1], to(0, True)).start()

    def wait_ag(g, d):
        here = nwg.at[g, c, d]
        remote(here, here, sem_send.at[2], sem_ag.at[g, d], to(0, True)).wait_recv()

    def wait_ad(g, k):
        here = nwd.at[g, c, k]
        remote(here, here, sem_send.at[4], sem_ad.at[g, k], to(0, True)).wait_recv()

    def own_copies(g):
        slot = g % OWN
        return (
            functools.partial(pltpu.make_async_remote_copy,
                own_g.at[slot, 1 - c], p_g.at[g % RING], sem_own.at[slot, 0], sem_pg.at[g], device_id=to(0, True), device_id_type=MESH),
            functools.partial(pltpu.make_async_remote_copy,
                own_d.at[slot, 1 - c], p_d.at[g % RING], sem_own.at[slot, 1], sem_pd.at[g], device_id=to(0, True), device_id_type=MESH),
        )

    def sum_of(*terms):
        out = terms[0].astype(F32)
        for one in terms[1:]:
            out = out + one.astype(F32)
        return out.astype(BF)

    def sum_g(g, j, *more):
        return sum_of(own_g[g % OWN, c, j], p_g[g % RING, j], *more)

    def sum_d(g, k, *more):
        return sum_of(own_d[g % OWN, c, k], p_d[g % RING, k], *more)

    def dest_of(g, k):
        return down_piece(g % NL, c, k)[0]

    def final_g(g, rz):
        slot, layer, f = g % KEEP, 1 - g // NL, strips_of(g % NL)
        if rz == 1:
            wait_rg(g, z)
            wait_rg(g, 4)
            total = sum_g(g, z, nwg[g, c, z], x_g[g % RING])
        else:
            @pl.when(z == 0)
            def _():
                wait_rg(g, 4)
                nwg[g, c, z] = x_g[g % RING]

            @pl.when(z == 3)
            def _():
                wait_rg(g, z)

            total = sum_g(g, z, nwg[g, c, z])
        for j in range(4):
            q, k = j // 2, j % 2
            rows, cols, at = slice(80 * q, 80 * q + 80), slice(S * k, S * k + S), pl.ds(f[k], S)
            om, ov = ((omg, ovg), (omu, ovu))[q]
            w = st_wg[slot, :, C * q + S * k : C * q + S * k + S].astype(F32)
            new, m, v = adamw(w, om[layer, :, at], ov[layer, :, at], total[rows, cols].astype(F32))
            nwg[g, c, z, rows, cols] = new
            om[layer, :, at] = m
            ov[layer, :, at] = v
        if rz == 1:
            ag_start_g(g, z, 1)
            ag_start_g(g, z, -1)
        else:
            ag_start_g(g, z, jnp.where(z == 0, 1, -1))
        partner_start_g(g, z)

    def final_d(g, rz):
        slot, layer = g % KEEP, 1 - g // NL
        for k in range(2):
            @pl.when(dest_of(g, k) == z)
            def _():
                if rz == 1:
                    wait_rd(g, k, 0)
                    wait_rd(g, k, 1)
                    total = sum_d(g, k, nwd[g, c, k], x_d[g // 2 % (RING // 2), k])
                else:
                    @pl.when(z == 0)
                    def _():
                        wait_rd(g, k, 1)
                        nwd[g, c, k] = x_d[g // 2 % (RING // 2), k]

                    @pl.when(z == 3)
                    def _():
                        wait_rd(g, k, 0)

                    total = sum_d(g, k, nwd[g, c, k])
                at = pl.ds(down_piece(g % NL, c, k)[1], 64)
                new, m, v = adamw(st_wd[slot, k].astype(F32), omd[layer, at, :], ovd[layer, at, :], total.astype(F32))
                nwd[g, c, k] = new
                omd[layer, at, :] = m
                ovd[layer, at, :] = v
                if rz == 1:
                    ag_start_d(g, k, 1)
                    ag_start_d(g, k, -1)
                else:
                    ag_start_d(g, k, jnp.where(z == 0, 1, -1))
                partner_start_d(g, k)

    def mirrored(rz, rd):
        plain = z == rz
        return plain | (z == 3 - rz), jnp.where(plain, rd, 3 - rd), jnp.where(plain, 1, -1), jnp.where(plain, 0, 1)

    def reduce_step(g, kind, rz, rd):
        active, d, dz, side = mirrored(rz, rd)
        if kind == "g":
            @pl.when(active)
            def _():
                if rz == 0:
                    p_g[g % RING, d] = sum_g(g, d)
                else:
                    wait_rg(g, d)
                    p_g[g % RING, d] = sum_g(g, d, nwg[g, c, d])
                rs_start_g(g, d, dz)
            return
        for k in range(2):
            @pl.when(active & (dest_of(g, k) == d))
            def _():
                if rz == 0:
                    p_d[g % RING, k] = sum_d(g, k)
                else:
                    wait_rd(g, k, side)
                    p_d[g % RING, k] = sum_d(g, k, nwd[g, c, k])
                rs_start_d(g, k, d, dz)

    def final_step(g, kind, rz):
        final = final_g if kind == "g" else final_d
        pl.when((z == rz) | (z == 3 - rz))(lambda: final(g, rz))

    def gather_step(g, kind, rz, rd):
        active, d, dz, _ = mirrored(rz, rd)
        if kind == "g":
            @pl.when(active)
            def _():
                wait_ag(g, d)
                if rz < 3:
                    ag_start_g(g, d, dz)
                partner_start_g(g, d)
            return
        for k in range(2):
            @pl.when(active & (dest_of(g, k) == d))
            def _():
                wait_ad(g, k)
                if rz < 3:
                    ag_start_d(g, k, dz)
                partner_start_d(g, k)

    def partner_step(g, kind, rz):
        one = own_copies(g)["gd".index(kind)]
        pl.when((z == rz) | (z == 3 - rz))(lambda: one().wait_recv())

    def sums_sent(g):
        slot = g % RING

        def wait(ref, at):
            remote(ref, ref, sem_rs.at[slot, at], sem_pa.at[0], to(0, True)).wait_send()

        for j in range(4):
            pl.when(z != j)(lambda j=j: wait(p_g.at[slot, j], j))
        for k in range(2):
            pl.when(dest_of(g, k) != z)(lambda k=k: wait(p_d.at[slot, k], 4 + k))

    def own_sent(g):
        for one in own_copies(g):
            one().wait_send()

    steps = {"partner": partner_step, "sum": reduce_step, "final": final_step, "gather": gather_step, "sent": own_sent, "sums_sent": sums_sent}

    def tick(it, s):
        todo = [((FIRST + o) // PARTS, n, step) for n, (*step, o) in enumerate(SCHEDULE) if (FIRST + o) % PARTS == s]
        for lag, _, (name, *rest) in sorted(todo, key=lambda one: (-one[0], one[1])):
            when_chunk(it - lag, functools.partial(lambda g, name, rest: steps[name](g, *rest), name=name, rest=rest))

    def when_chunk(g, fn):
        pl.when((g >= 0) & (g < NG))(lambda: fn(g))

    NT = T // TILE

    def tile_of(i):
        return pl.ds(pl.multiple_of(i * TILE, TILE), TILE)

    def tile_in(src, i):
        return pltpu.make_async_copy(src.at[tile_of(i)], A.at[tile_of(i)], sem_in.at[i])

    def tiles_in(src):
        @pl.loop(0, NT)
        def _(i):
            tile_in(src, i).start()

    def h_parts(i):
        rows = tile_of(i)
        return (DGU.at[rows], pl.ds(0, 512)), (HID.at[rows, pl.ds(0, 128)], pl.ds(512, 128))

    def x_again(i):
        return [functools.partial(pltpu.make_async_copy, x_h.at[tile_of(i), cols], ref, sem_h.at[0, i, k]) for k, (ref, cols) in enumerate(h_parts(i))]

    def h1_out(i):
        return [functools.partial(pltpu.make_async_copy, ref, h1_h.at[tile_of(i), cols], sem_h.at[1, i, k]) for k, (ref, cols) in enumerate(h_parts(i))]

    def each(copies, act):
        for one in copies:
            getattr(one(), act)()

    y_in = pltpu.make_async_copy(dy_h, Y, sem_in.at[NT + 1])
    tile_in(x_h, 0).start()
    w_start(0)
    w_start(1)
    for t in range(1, NT):
        tile_in(x_h, t).start()
    a_out = pltpu.make_async_copy(A, a0_h, sem_in.at[NT])

    def forward_tile(n, t):
        rows = pl.ds(t * TILE, TILE) if isinstance(t, int) else tile_of(t)
        a = A[rows, :]
        total = 0.0
        for slot in ((2 * n) % WS, (2 * n + 1) % WS):
            both = dot(a, WGU[slot])
            gate, up = both[:, :C], both[:, C:]
            hid = (gate * jax.nn.sigmoid(gate) * up).astype(BF)
            total = total + dot(hid, WD[slot])
        return rows, total

    def turn(src, dst):
        @pl.loop(0, NT)
        def _(t):
            rows = tile_of(t)
            dst[:, rows] = src[rows, :].T

    def forward_weights(n):
        w_wait(2 * n)
        w_wait(2 * n + 1)
        w_start(2 * n + 2)
        w_start(2 * n + 3)

    for t in range(NT):
        tile_in(x_h, t).wait()
        rows = pl.ds(t * TILE, TILE)
        wide, scale = norm_of(A[rows, :])
        A[rows, :] = (wide * scale).astype(BF)
        if t == 0:
            forward_weights(0)
        rows, total = forward_tile(0, t)
        ACC[rows, :] = total
    a_out.start()
    y_in.start()
    for t in range(NT):
        each(x_again(t), "start")
    each(moments_in(), "start")

    @pl.loop(1, NL // 2 - 1)
    def _(n):
        forward_weights(n)
        for t in range(NT):
            rows, total = forward_tile(n, t)
            ACC[rows, :] += total

    a_out.wait()
    forward_weights(NL // 2 - 1)
    for t in range(NT):
        each(x_again(t), "wait")
    def last_forward(t):
        rows, total = forward_tile(NL // 2 - 1, t)
        ACC[rows, :] += total

    def layer_input(t):
        rows = pl.ds(t * TILE, TILE)
        total = ACC[rows, :].astype(BF).astype(F32)
        ACC[rows, :] = jnp.zeros((TILE, D), F32)
        ha = (DGU[rows, :].astype(F32) + total[:, :512]).astype(BF)
        hb = (HID[rows, :128].astype(F32) + total[:, 512:]).astype(BF)
        DGU[rows, :] = ha
        HID[rows, :128] = hb
        ha, hb = ha.astype(F32), hb.astype(F32)
        mean = (jnp.sum(ha * ha, -1, keepdims=True) + jnp.sum(hb * hb, -1, keepdims=True)) * (1.0 / D)
        scale = lax.rsqrt(mean + EPS)
        A[rows, :512] = (ha * scale).astype(BF)
        A[rows, 512:] = (hb * scale).astype(BF)
        AT[:, rows] = A[rows, :].T
        YT[:, rows] = Y[rows, :].T

    y_in.wait()
    last_forward(0)

    for t in range(1, NT):
        last_forward(t)
        layer_input(t - 1)
    layer_input(NT - 1)

    @pl.loop(0, NT)
    def _(t):
        each(h1_out(t), "start")

    each(moments_in(), "wait")
    pl.semaphore_wait(barrier, 1 + jnp.where(z > 0, 1, 0) + jnp.where(z < 3, 1, 0))

    def tiles(g, first, last):
        slot = (g + NL) % WS
        for t in range(first, last):
            rows = pl.ds(t * TILE, TILE)
            both = dot(A[rows, :], WGU[slot])
            gate, up = both[:, :C], both[:, C:]
            by_hid = dot_t(Y[rows, :], WD[slot]).astype(BF).astype(F32)
            sig = jax.nn.sigmoid(gate)
            silu = gate * sig
            HID[rows, :] = (silu * up).astype(BF)
            DGU[rows, C:] = (by_hid * silu).astype(BF)
            DGU[rows, :C] = (by_hid * up * (sig + silu * (1.0 - sig))).astype(BF)

    def input_grad(g):
        slot = (g + NL) % WS
        for t in range(NT):
            rows = pl.ds(t * TILE, TILE)
            ACC[rows, :] += dot_t(DGU[rows, :], WGU[slot])

    def layer_change(slot, first):
        for t in range(2):
            tile_in(h1_h, first + t).wait()

        @pl.loop(first, first + 2)
        def _(t):
            rows = tile_of(t)
            ct = (ACC[rows, :] + dot_t(DGU[rows, :], WGU[slot])).astype(BF).astype(F32)
            wide, scale = norm_of(A[rows, :])
            by_scale = jnp.sum(ct * wide, -1, keepdims=True)
            by_h = ct * scale - wide * (by_scale * scale * scale * scale * (1.0 / D))
            y = (Y[rows, :].astype(F32) + by_h.astype(BF).astype(F32)).astype(BF)
            Y[rows, :] = y
            YT[:, rows] = y.T
            tile_in(a0_h, t).start()

    def weight_grads(g):
        slot = g % OWN
        out = dot(AT[...], DGU[...]).astype(BF)
        for q in range(2):
            for b in range(8):
                own_g[slot, b % 2, b // 2, 80 * q : 80 * q + 80, :] = out[80 * b : 80 * b + 80, C * q : C * q + C]

    def down_grad(g):
        slot = g % OWN
        out = dot(YT[...], HID[...]).T.astype(BF)
        mid = (g % NL) // 2 == 2
        for strip in range(2):
            for half in range(2):
                core = jnp.where(mid, half, strip)
                k = jnp.where(mid, strip, half)
                row = S * strip + 64 * half
                own_d[slot, core, k] = out[row : row + 64, :]

    def part(g, s):
        if s == 0:
            w_wait(g + NL)
            pl.when(g + 2 < NG)(lambda: w_start(g + NL + 2))

            @pl.when(g == 0)
            def _():
                for t in range(NT):
                    each(h1_out(t), "wait")

            @pl.when(g == NL)
            def _():
                layer_change((2 * NL - 1) % WS, 2)
                for t in range(2):
                    tile_in(a0_h, t).wait()

            keep_weights(g)
            tiles(g, 0, 2)
        elif s == 1:
            @pl.when(g == NL)
            def _():
                for t in range(2, NT):
                    tile_in(a0_h, t).wait()

            tiles(g, 2, 4)
            pl.when(g == NL - 1)(lambda: tiles_in(h1_h))
        elif s == 2:
            pl.when(g == NL)(lambda: turn(A, AT))
            weight_grads(g)
            own_copies(g)[0]().start()
        elif s == 3:
            down_grad(g)
            own_copies(g)[1]().start()
        else:
            pl.when(g < NL - 1)(lambda: input_grad(g))
            pl.when(g == NL - 1)(lambda: layer_change((2 * NL - 1) % WS, 0))

    @pl.loop(0, NG + LAST)
    def _(g):
        for s in range(PARTS):
            pl.when(g < NG)(functools.partial(part, g, s))
            tick(g, s)

    def all_of(ref, send, recv):
        return remote(ref, ref, send, recv, to(0, True))

    all_of(nwg.at[:, 1 - c], sem_send.at[6], sem_pa.at[0]).wait_recv()
    all_of(nwd.at[:, 1 - c], sem_send.at[7], sem_pa.at[1]).wait_recv()

    def sent(which, ref):
        all_of(ref, sem_send.at[which], sem_pa.at[0]).wait_send()

    sent(6, nwg.at[:, c])
    sent(7, nwd.at[:, c])

    for zz in range(4):
        right, left = ((1, 0), (2, 3), (3, 2), (0, 1))[zz]

        @pl.when(z == zz)
        def _():
            if right:
                sent(2, nwg.at[:, 0, pl.ds(0, right)])
                sent(4, nwd.at[pl.ds(0, 5 * right), 0])
            if left:
                sent(3, nwg.at[:, 0, pl.ds(0, left)])
                sent(5, nwd.at[pl.ds(0, 5 * left), 0])


def train(x, dy, *arrays):
    anyspace = pl.BlockSpec(memory_space=pl.ANY)
    sds = jax.ShapeDtypeStruct
    dma = pltpu.SemaphoreType.DMA
    vm = pltpu.VMEM
    outs = (
        vm((NG, 2, 4, 160, C), BF), vm((NG, 2, 2, 64, D), BF),
        vm((2, 80, FF), F32), vm((2, 80, FF), F32), vm((2, 320, D), F32),
        vm((2, 80, FF), F32), vm((2, 80, FF), F32), vm((2, 320, D), F32),
        sds((T, D), BF), sds((T, D), BF),
    )
    return pl.pallas_call(
        kernel,
        out_shape=outs,
        in_specs=[anyspace] * 11,
        out_specs=(pl.BlockSpec(memory_space=pltpu.VMEM),) * 8 + (anyspace,) * 2,
        scratch_shapes=[
            vm((T, D), BF), vm((D, T), BF), vm((T, D), BF), vm((D, T), BF), vm((T, D), F32),
            vm((T, C), BF), vm((T, 2 * C), BF), vm((WS, D, 2 * C), BF), vm((WS, C, D), BF),
            vm((OWN, 2, 4, 160, C), BF), vm((OWN, 2, 2, 64, D), BF),
            vm((RING, 4, 160, C), BF), vm((RING, 2, 64, D), BF), vm((RING, 160, C), BF), vm((RING // 2, 2, 64, D), BF),
            vm((KEEP, 80, 2 * C), BF), vm((KEEP, 2, 64, D), BF),
            dma((10,)), dma((WS, 6)), dma((6,)), dma((8,)), dma((RING, 6)), dma((2, 4, 2)), dma((OWN, 2)), dma((NG,)), dma((NG,)),
            dma((NG, 5)), dma((NG, 2, 2)), dma((NG, 4)), dma((NG, 2)), dma((2,)),
        ],
        compiler_params=pltpu.CompilerParams(
            collective_id=0, has_side_effects=True, vmem_limit_bytes=37500000),
        name="train",
    )(x, dy, *arrays)


def place(nwg, nwd, *refs):
    moments, (wg, wu, wd), outs, (sem_out, sem_mo) = refs[:6], refs[6:9], refs[9:15], refs[15:]

    def moment(j):
        return pltpu.make_async_copy(moments[j], outs[j], sem_mo.at[j])

    def store(g, act):
        layer, i = 1 - g // NL, g % NL
        f = strips_of(i)

        @pl.loop(0, 8)
        def _(b):
            rows = pl.ds(pl.multiple_of(80 * b, 80), 80)
            for q, out in enumerate((wg, wu)):
                for k in range(2):
                    src = nwg.at[g, b % 2, b // 2, pl.ds(80 * q, 80), pl.ds(S * k, S)]
                    getattr(pltpu.make_async_copy(src, out.at[layer, rows, pl.ds(f[k], S)], sem_out.at[0]), act)()

        for core in range(2):
            for k in range(2):
                dest, off = down_piece(i, core, k)
                rows = pl.ds(pl.multiple_of(640 * dest + 320 * core + off, 64), 64)
                getattr(pltpu.make_async_copy(nwd.at[g, core, k], wd.at[layer, rows], sem_out.at[1]), act)()

    for j in range(6):
        moment(j).start()

    @pl.loop(0, NG)
    def _(g):
        store(g, "start")

    for j in range(6):
        moment(j).wait()

    @pl.loop(0, NG)
    def _(g):
        store(g, "wait")


def finish(*arrays):
    anyspace = pl.BlockSpec(memory_space=pl.ANY)
    sds = jax.ShapeDtypeStruct
    dma = pltpu.SemaphoreType.DMA
    moments = [sds(one.shape, one.dtype) for one in arrays[2:]]
    return pl.pallas_call(
        place,
        out_shape=(sds((2, D, FF), BF), sds((2, D, FF), BF), sds((2, FF, D), BF), *moments),
        in_specs=[pl.BlockSpec(memory_space=pltpu.VMEM)] * 8,
        out_specs=(anyspace,) * 9,
        scratch_shapes=[
            dma((2,)), dma((6,)),
        ],
        compiler_params=pltpu.CompilerParams(vmem_limit_bytes=2000000),
        name="place",
    )(*(pltpu.with_memory_space_constraint(one, pltpu.VMEM) for one in arrays))


def solution(mesh):
    def step(x, dy, *arrays):
        return finish(*train(x[0], dy[0], *arrays)[:8])

    whole = P(None, None, None)
    rows = P(None, "dp", None)
    seq = P(("rep", "dp"), None, None)
    return jax.shard_map(
        step,
        mesh=mesh,
        in_specs=(seq, seq) + (whole,) * 3 + (rows,) * 6,
        out_specs=(P("rep", None, None),) * 3 + (P("rep", "dp", None),) * 6,
        check_vma=False,
    )
```

```python
import functools

import jax
import jax.numpy as jnp
from jax import lax
from jax.experimental import pallas as pl
from jax.experimental.pallas import tpu as pltpu
from jax.sharding import PartitionSpec as P

MESH = pl.DeviceIdType.MESH
BF = jnp.bfloat16
F32 = jnp.float32
T, D, FF = 2048, 640, 2560
C = 256
S = 128
NL = 10
NG = 20
TILE = 512
EPS = 1e-6
WS = 4
OWN = 3
KEEP = 4
RING = 6
PARTS = 5
FIRST = 2
TIMES = (
    ("partner", (0,), 1, 1),
    ("partner", (1,), 4, 6),
    ("sum", (0, 3,), 1, 2),
    ("sum", (0, 2,), 1, 1),
    ("sum", (0, 1,), 5, 3),
    ("sum", (1, 3,), 4, 7),
    ("sum", (1, 2,), 5, 6),
    ("sum", (2, 3,), 7, 9),
    ("final", (1,), 8, 9),
    ("final", (0,), 13, 14),
    ("gather", (2, 1,), 11, 12),
    ("gather", (1, 0,), 17, 18),
    ("gather", (3, 1,), 13, 23),
    ("gather", (2, 0,), 20, 20),
    ("gather", (3, 0,), 25, 29),
    ("gather", (3, 2,), 20, 24),
)
SCHEDULE = [(step, kind, *chips, when) for step, chips, *both in TIMES for kind, when in zip("gd", both)]
SCHEDULE += [("sent", 12), ("sums_sent", 18)]
LAST = max((FIRST + one[-1]) // PARTS for one in SCHEDULE)


def chunk_of(i):
    pair, t = i % 2, i // 2
    low = t <= 2
    z1, s1 = jnp.where(low, pair, 3 - pair), jnp.where(low, t, 4 - t)
    z2, s2 = jnp.where(low, 3 - pair, pair), jnp.where(low, 4 - t, t)
    return t, z1, s1, z2, s2


def strips_of(i):
    _, z1, s1, z2, s2 = chunk_of(i)
    return pl.multiple_of(640 * z1 + S * s1, S), pl.multiple_of(640 * z2 + S * s2, S)


def down_piece(i, c, k):
    t, z1, s1, z2, s2 = chunk_of(i)
    mid = t == 2
    dest = jnp.where(mid, z1 if k == 0 else z2, jnp.where(c == 0, z1, z2))
    s = jnp.where(c == 0, s1, s2)
    off = jnp.where(mid, jnp.where(c == 0, 256, 0), 64 * (2 * s + k - 5 * c))
    return dest, pl.multiple_of(off, 64)


def norm_of(h):
    wide = h.astype(F32)
    scale = lax.rsqrt(jnp.mean(wide * wide, -1, keepdims=True) + EPS)
    return wide, scale


def dot(a, b):
    return jnp.dot(a, b, preferred_element_type=F32)


def dot_t(a, b):
    return lax.dot_general(a, b, (((1,), (1,)), ((), ())), preferred_element_type=F32)


def adamw(w, m, v, g):
    m = 0.9 * m + 0.1 * g
    v = 0.95 * v + 0.05 * g * g
    step = m * lax.rsqrt(v + 1e-8) + 0.1 * w
    return (w - 0.02 * step).astype(BF), m, v


def kernel(
    x_h, dy_h, wg_h, wu_h, wd_h, mg_h, mu_h, md_h, vg_h, vu_h, vd_h,
    nwg, nwd, omg, omu, omd, ovg, ovu, ovd, a0_h, h1_h,
    A, AT, Y, YT, ACC, HID, DGU, WGU, WD, own_g, own_d, p_g, p_d, x_g, x_d,
    st_wg, st_wd,
    sem_in, sem_w, sem_ld, sem_send, sem_rs, sem_h, sem_own, sem_pg, sem_pd, sem_rg, sem_rd, sem_ag, sem_ad, sem_pa,
):
    rep, dp = lax.axis_index("rep"), lax.axis_index("dp")
    z, c = dp // 2, dp % 2
    is_end = (z == 0) | (z == 3)
    is_mid = (z == 1) | (z == 2)

    def to(dz, flip=False):
        return (rep, (z + dz) * 2 + ((1 - c) if flip else c))

    def other_core():
        return to(0, True)

    barrier = pltpu.get_barrier_semaphore()
    pl.semaphore_signal(barrier, inc=1, device_id=other_core(), device_id_type=MESH)

    @pl.when(z > 0)
    def _():
        pl.semaphore_signal(barrier, inc=1, device_id=to(-1), device_id_type=MESH)

    @pl.when(z < 3)
    def _():
        pl.semaphore_signal(barrier, inc=1, device_id=to(1), device_id_type=MESH)

    def w_copies(n):
        layer = jnp.where((n >= 10) & (n < 20), 1, 0)
        slot = n % WS
        out = []
        for k, f in enumerate(strips_of(n % NL)):
            out.append(functools.partial(pltpu.make_async_copy, wg_h.at[layer, :, pl.ds(f, S)], WGU.at[slot, :, pl.ds(S * k, S)], sem_w.at[slot, k]))
            out.append(functools.partial(pltpu.make_async_copy, wu_h.at[layer, :, pl.ds(f, S)], WGU.at[slot, :, pl.ds(C + S * k, S)], sem_w.at[slot, 2 + k]))
            out.append(functools.partial(pltpu.make_async_copy, wd_h.at[layer, pl.ds(f, S), :], WD.at[slot, pl.ds(S * k, S), :], sem_w.at[slot, 4 + k]))
        return out

    def w_start(n):
        for one in w_copies(n):
            one().start()

    def w_wait(n):
        for one in w_copies(n):
            one().wait()

    def moments_in():
        return [functools.partial(pltpu.make_async_copy, src, dst, sem_ld.at[n])
                for n, (src, dst) in enumerate(((mg_h, omg), (mu_h, omu), (md_h, omd), (vg_h, ovg), (vu_h, ovu), (vd_h, ovd)))]

    def keep_weights(g):
        slot, w = g % KEEP, (g + NL) % WS
        st_wg[slot] = WGU[w, pl.ds(pl.multiple_of(80 * dp, 16), 80), :]
        mid = (g % NL) // 2 == 2
        for k in range(2):
            @pl.when(dest_of(g, k) == z)
            def _():
                row = jnp.where(mid, S * k + 64 * c, S * c + 64 * k)
                st_wd[slot, k] = WD[w, pl.ds(pl.multiple_of(row, 64), 64), :]

    def remote(src, dst, send, recv, where):
        return pltpu.make_async_remote_copy(src, dst, send, recv, device_id=where, device_id_type=MESH)

    def rs_start_g(g, j, dz):
        to_end = (dz == -1) & (j == z - 1)

        @pl.when(to_end)
        def _():
            remote(p_g.at[g % RING, j], x_g.at[g % RING], sem_rs.at[g % RING, j], sem_rg.at[g, 4], to(-1)).start()

        @pl.when(jnp.logical_not(to_end))
        def _():
            remote(p_g.at[g % RING, j], nwg.at[g, c, j], sem_rs.at[g % RING, j], sem_rg.at[g, j], to(dz)).start()

    def rs_start_d(g, k, d, dz):
        to_end = (dz == -1) & (d == z - 1)

        @pl.when(to_end)
        def _():
            remote(p_d.at[g % RING, k], x_d.at[g // 2 % (RING // 2), k], sem_rs.at[g % RING, 4 + k], sem_rd.at[g, k, 1], to(-1)).start()

        @pl.when(jnp.logical_not(to_end))
        def _():
            side = jnp.where(dz == 1, 0, 1)
            remote(p_d.at[g % RING, k], nwd.at[g, c, k], sem_rs.at[g % RING, 4 + k], sem_rd.at[g, k, side], to(dz)).start()

    def wait_rg(g, slot):
        remote(p_g.at[g % RING, 0], x_g.at[g % RING], sem_send.at[0], sem_rg.at[g, slot], other_core()).wait_recv()

    def wait_rd(g, k, side):
        remote(p_d.at[g % RING, k], x_d.at[g // 2 % (RING // 2), k], sem_send.at[1], sem_rd.at[g, k, side], other_core()).wait_recv()

    def ag_start_g(g, d, dz):
        here = nwg.at[g, c, d]
        remote(here, here, sem_send.at[jnp.where(dz == 1, 2, 3)], sem_ag.at[g, d], to(dz)).start()

    def ag_start_d(g, k, dz):
        here = nwd.at[g, c, k]
        remote(here, here, sem_send.at[jnp.where(dz == 1, 4, 5)], sem_ad.at[g, k], to(dz)).start()

    def partner_start_g(g, d):
        here = nwg.at[g, c, d]
        remote(here, here, sem_send.at[6], sem_pa.at[0], other_core()).start()

    def partner_start_d(g, k):
        here = nwd.at[g, c, k]
        remote(here, here, sem_send.at[7], sem_pa.at[1], other_core()).start()

    def wait_ag(g, d):
        here = nwg.at[g, c, d]
        remote(here, here, sem_send.at[2], sem_ag.at[g, d], other_core()).wait_recv()

    def wait_ad(g, k):
        here = nwd.at[g, c, k]
        remote(here, here, sem_send.at[4], sem_ad.at[g, k], other_core()).wait_recv()

    def own_copies(g):
        slot = g % OWN
        return (
            functools.partial(pltpu.make_async_remote_copy,
                own_g.at[slot, 1 - c], p_g.at[g % RING], sem_own.at[slot, 0], sem_pg.at[g], device_id=other_core(), device_id_type=MESH),
            functools.partial(pltpu.make_async_remote_copy,
                own_d.at[slot, 1 - c], p_d.at[g % RING], sem_own.at[slot, 1], sem_pd.at[g], device_id=other_core(), device_id_type=MESH),
        )

    def sum_of(*terms):
        out = terms[0].astype(F32)
        for one in terms[1:]:
            out = out + one.astype(F32)
        return out.astype(BF)

    def sum_g(g, j, *more):
        return sum_of(own_g[g % OWN, c, j], p_g[g % RING, j], *more)

    def sum_d(g, k, *more):
        return sum_of(own_d[g % OWN, c, k], p_d[g % RING, k], *more)

    def dest_of(g, k):
        return down_piece(g % NL, c, k)[0]

    def final_g(g, rz):
        slot, layer, f = g % KEEP, 1 - g // NL, strips_of(g % NL)
        if rz == 1:
            wait_rg(g, z)
            wait_rg(g, 4)
            total = sum_g(g, z, nwg[g, c, z], x_g[g % RING])
        else:
            @pl.when(z == 0)
            def _():
                wait_rg(g, 4)
                nwg[g, c, z] = x_g[g % RING]

            @pl.when(z == 3)
            def _():
                wait_rg(g, z)

            total = sum_g(g, z, nwg[g, c, z])
        for j in range(4):
            q, k = j // 2, j % 2
            rows, cols, at = slice(80 * q, 80 * q + 80), slice(S * k, S * k + S), pl.ds(f[k], S)
            om, ov = ((omg, ovg), (omu, ovu))[q]
            w = st_wg[slot, :, C * q + S * k : C * q + S * k + S].astype(F32)
            new, m, v = adamw(w, om[layer, :, at], ov[layer, :, at], total[rows, cols].astype(F32))
            nwg[g, c, z, rows, cols] = new
            om[layer, :, at] = m
            ov[layer, :, at] = v
        if rz == 1:
            ag_start_g(g, z, 1)
            ag_start_g(g, z, -1)
        else:
            ag_start_g(g, z, jnp.where(z == 0, 1, -1))
        partner_start_g(g, z)

    def final_d(g, rz):
        slot, layer = g % KEEP, 1 - g // NL
        for k in range(2):
            @pl.when(dest_of(g, k) == z)
            def _():
                if rz == 1:
                    wait_rd(g, k, 0)
                    wait_rd(g, k, 1)
                    total = sum_d(g, k, nwd[g, c, k], x_d[g // 2 % (RING // 2), k])
                else:
                    @pl.when(z == 0)
                    def _():
                        wait_rd(g, k, 1)
                        nwd[g, c, k] = x_d[g // 2 % (RING // 2), k]

                    @pl.when(z == 3)
                    def _():
                        wait_rd(g, k, 0)

                    total = sum_d(g, k, nwd[g, c, k])
                at = pl.ds(down_piece(g % NL, c, k)[1], 64)
                new, m, v = adamw(st_wd[slot, k].astype(F32), omd[layer, at, :], ovd[layer, at, :], total.astype(F32))
                nwd[g, c, k] = new
                omd[layer, at, :] = m
                ovd[layer, at, :] = v
                if rz == 1:
                    ag_start_d(g, k, 1)
                    ag_start_d(g, k, -1)
                else:
                    ag_start_d(g, k, jnp.where(z == 0, 1, -1))
                partner_start_d(g, k)

    def mirrored(rz, rd):
        plain = z == rz
        return plain | (z == 3 - rz), jnp.where(plain, rd, 3 - rd), jnp.where(plain, 1, -1), jnp.where(plain, 0, 1)

    def reduce_step(g, kind, rz, rd):
        active, d, dz, side = mirrored(rz, rd)
        if kind == "g":
            @pl.when(active)
            def _():
                if rz == 0:
                    p_g[g % RING, d] = sum_g(g, d)
                else:
                    wait_rg(g, d)
                    p_g[g % RING, d] = sum_g(g, d, nwg[g, c, d])
                rs_start_g(g, d, dz)
            return
        for k in range(2):
            @pl.when(active & (dest_of(g, k) == d))
            def _():
                if rz == 0:
                    p_d[g % RING, k] = sum_d(g, k)
                else:
                    wait_rd(g, k, side)
                    p_d[g % RING, k] = sum_d(g, k, nwd[g, c, k])
                rs_start_d(g, k, d, dz)

    def final_step(g, kind, rz):
        final = final_g if kind == "g" else final_d
        pl.when((z == rz) | (z == 3 - rz))(lambda: final(g, rz))

    def gather_step(g, kind, rz, rd):
        active, d, dz, _ = mirrored(rz, rd)
        if kind == "g":
            @pl.when(active)
            def _():
                wait_ag(g, d)
                if rz < 3:
                    ag_start_g(g, d, dz)
                partner_start_g(g, d)
            return
        for k in range(2):
            @pl.when(active & (dest_of(g, k) == d))
            def _():
                wait_ad(g, k)
                if rz < 3:
                    ag_start_d(g, k, dz)
                partner_start_d(g, k)

    def partner_step(g, kind, rz):
        one = own_copies(g)["gd".index(kind)]
        pl.when((z == rz) | (z == 3 - rz))(lambda: one().wait_recv())

    def sums_sent(g):
        slot = g % RING

        def wait(ref, at):
            remote(ref, ref, sem_rs.at[slot, at], sem_pa.at[0], other_core()).wait_send()

        for j in range(4):
            pl.when(z != j)(lambda j=j: wait(p_g.at[slot, j], j))
        for k in range(2):
            pl.when(dest_of(g, k) != z)(lambda k=k: wait(p_d.at[slot, k], 4 + k))

    def own_sent(g):
        for one in own_copies(g):
            one().wait_send()

    steps = {"partner": partner_step, "sum": reduce_step, "final": final_step, "gather": gather_step, "sent": own_sent, "sums_sent": sums_sent}

    def tick(it, s):
        todo = [((FIRST + o) // PARTS, n, step) for n, (*step, o) in enumerate(SCHEDULE) if (FIRST + o) % PARTS == s]
        for lag, _, (name, *rest) in sorted(todo, key=lambda one: (-one[0], one[1])):
            when_chunk(it - lag, functools.partial(lambda g, name, rest: steps[name](g, *rest), name=name, rest=rest))

    def when_chunk(g, fn):
        pl.when((g >= 0) & (g < NG))(lambda: fn(g))

    NT = T // TILE

    def tile_of(i):
        return pl.ds(pl.multiple_of(i * TILE, TILE), TILE)

    def tile_in(src, i):
        return pltpu.make_async_copy(src.at[tile_of(i)], A.at[tile_of(i)], sem_in.at[i])

    def tiles_in(src):
        @pl.loop(0, NT)
        def _(i):
            tile_in(src, i).start()

    def h_parts(i):
        rows = tile_of(i)
        return (DGU.at[rows], pl.ds(0, 512)), (HID.at[rows, pl.ds(0, 128)], pl.ds(512, 128))

    def x_again(i):
        return [functools.partial(pltpu.make_async_copy, x_h.at[tile_of(i), cols], ref, sem_h.at[0, i, k]) for k, (ref, cols) in enumerate(h_parts(i))]

    def h1_out(i):
        return [functools.partial(pltpu.make_async_copy, ref, h1_h.at[tile_of(i), cols], sem_h.at[1, i, k]) for k, (ref, cols) in enumerate(h_parts(i))]

    def each(copies, act):
        for one in copies:
            getattr(one(), act)()

    y_in = pltpu.make_async_copy(dy_h, Y, sem_in.at[NT + 1])
    tile_in(x_h, 0).start()
    w_start(0)
    w_start(1)
    for t in range(1, NT):
        tile_in(x_h, t).start()
    a_out = pltpu.make_async_copy(A, a0_h, sem_in.at[NT])

    def forward_tile(n, t, size=TILE):
        rows = pl.ds(t * size, size)
        a = A[rows, :]
        total = 0.0
        for slot in ((2 * n) % WS, (2 * n + 1) % WS):
            both = dot(a, WGU[slot])
            gate, up = both[:, :C], both[:, C:]
            hid = (gate * jax.nn.sigmoid(gate) * up).astype(BF)
            total = total + dot(hid, WD[slot])
        return rows, total

    def turn(src, dst):
        @pl.loop(0, NT)
        def _(t):
            rows = tile_of(t)
            dst[:, rows] = src[rows, :].T

    def forward_weights(n):
        w_wait(2 * n)
        w_wait(2 * n + 1)
        w_start(2 * n + 2)
        w_start(2 * n + 3)

    for t in range(NT):
        tile_in(x_h, t).wait()
        rows = pl.ds(t * TILE, TILE)
        wide, scale = norm_of(A[rows, :])
        A[rows, :] = (wide * scale).astype(BF)
        if t == 0:
            forward_weights(0)
        rows, total = forward_tile(0, t)
        ACC[rows, :] = total
    a_out.start()
    y_in.start()

    @pl.loop(1, NL // 2 - 1)
    def _(n):
        forward_weights(n)

        @pl.when(n == 2)
        def _():
            for t in range(NT):
                each(x_again(t), "start")

        pl.when(n == 3)(lambda: each(moments_in(), "start"))
        for t in range(NT // 2):
            rows, total = forward_tile(n, t, 2 * TILE)
            ACC[rows, :] += total

    a_out.wait()
    forward_weights(NL // 2 - 1)
    for t in range(NT):
        each(x_again(t), "wait")
    def last_forward(t):
        rows, total = forward_tile(NL // 2 - 1, t)
        ACC[rows, :] += total

    def layer_input(t):
        rows = pl.ds(t * TILE, TILE)
        total = ACC[rows, :].astype(BF).astype(F32)
        ACC[rows, :] = jnp.zeros((TILE, D), F32)
        ha = (DGU[rows, :].astype(F32) + total[:, :512]).astype(BF)
        hb = (HID[rows, :128].astype(F32) + total[:, 512:]).astype(BF)
        DGU[rows, :] = ha
        HID[rows, :128] = hb
        ha, hb = ha.astype(F32), hb.astype(F32)
        mean = (jnp.sum(ha * ha, -1, keepdims=True) + jnp.sum(hb * hb, -1, keepdims=True)) * (1.0 / D)
        scale = lax.rsqrt(mean + EPS)
        A[rows, :512] = (ha * scale).astype(BF)
        A[rows, 512:] = (hb * scale).astype(BF)
        AT[:, rows] = A[rows, :].T
        YT[:, rows] = Y[rows, :].T

    y_in.wait()
    last_forward(0)

    for t in range(1, NT):
        last_forward(t)
        layer_input(t - 1)
    layer_input(NT - 1)

    @pl.loop(0, NT)
    def _(t):
        each(h1_out(t), "start")

    each(moments_in(), "wait")
    pl.semaphore_wait(barrier, 1 + jnp.where(z > 0, 1, 0) + jnp.where(z < 3, 1, 0))

    def tiles(g, first, last):
        slot = (g + NL) % WS
        for t in range(first, last):
            rows = pl.ds(t * TILE, TILE)
            both = dot(A[rows, :], WGU[slot])
            gate, up = both[:, :C], both[:, C:]
            by_hid = dot_t(Y[rows, :], WD[slot]).astype(BF).astype(F32)
            sig = jax.nn.sigmoid(gate)
            silu = gate * sig
            HID[rows, :] = (silu * up).astype(BF)
            DGU[rows, C:] = (by_hid * silu).astype(BF)
            DGU[rows, :C] = (by_hid * up * (sig + silu * (1.0 - sig))).astype(BF)

    def input_grad(g):
        slot = (g + NL) % WS
        for t in range(NT):
            rows = pl.ds(t * TILE, TILE)
            ACC[rows, :] += dot_t(DGU[rows, :], WGU[slot])

    def layer_change(slot, first):
        for t in range(2):
            tile_in(h1_h, first + t).wait()

        @pl.loop(first, first + 2)
        def _(t):
            rows = tile_of(t)
            ct = (ACC[rows, :] + dot_t(DGU[rows, :], WGU[slot])).astype(BF).astype(F32)
            wide, scale = norm_of(A[rows, :])
            by_scale = jnp.sum(ct * wide, -1, keepdims=True)
            by_h = ct * scale - wide * (by_scale * scale * scale * scale * (1.0 / D))
            y = (Y[rows, :].astype(F32) + by_h.astype(BF).astype(F32)).astype(BF)
            Y[rows, :] = y
            YT[:, rows] = y.T
            tile_in(a0_h, t).start()

    def weight_grads(g):
        slot = g % OWN
        out = dot(AT[...], DGU[...]).astype(BF)
        for q in range(2):
            for b in range(8):
                own_g[slot, b % 2, b // 2, 80 * q : 80 * q + 80, :] = out[80 * b : 80 * b + 80, C * q : C * q + C]

    def down_grad(g):
        slot = g % OWN
        out = dot(YT[...], HID[...]).T.astype(BF)
        mid = (g % NL) // 2 == 2
        for strip in range(2):
            for half in range(2):
                core = jnp.where(mid, half, strip)
                k = jnp.where(mid, strip, half)
                row = S * strip + 64 * half
                own_d[slot, core, k] = out[row : row + 64, :]

    def part(g, s):
        if s == 0:
            w_wait(g + NL)
            pl.when(g + 2 < NG)(lambda: w_start(g + NL + 2))

            @pl.when(g == 0)
            def _():
                for t in range(NT):
                    each(h1_out(t), "wait")

            @pl.when(g == NL)
            def _():
                layer_change((2 * NL - 1) % WS, 2)
                for t in range(2):
                    tile_in(a0_h, t).wait()

            keep_weights(g)
            tiles(g, 0, 2)
        elif s == 1:
            @pl.when(g == NL)
            def _():
                for t in range(2, NT):
                    tile_in(a0_h, t).wait()

            tiles(g, 2, 4)
            pl.when(g == NL - 1)(lambda: tiles_in(h1_h))
        elif s == 2:
            pl.when(g == NL)(lambda: turn(A, AT))
            weight_grads(g)
            own_copies(g)[0]().start()
        elif s == 3:
            down_grad(g)
            own_copies(g)[1]().start()
        else:
            pl.when(g < NL - 1)(lambda: input_grad(g))
            pl.when(g == NL - 1)(lambda: layer_change((2 * NL - 1) % WS, 0))

    @pl.loop(0, NG + LAST)
    def _(g):
        for s in range(PARTS):
            pl.when(g < NG)(functools.partial(part, g, s))
            tick(g, s)

    def all_of(ref, send, recv):
        return remote(ref, ref, send, recv, other_core())

    all_of(nwg.at[:, 1 - c], sem_send.at[6], sem_pa.at[0]).wait_recv()
    all_of(nwd.at[:, 1 - c], sem_send.at[7], sem_pa.at[1]).wait_recv()

    def sent(which, ref):
        all_of(ref, sem_send.at[which], sem_pa.at[0]).wait_send()

    sent(6, nwg.at[:, c])
    sent(7, nwd.at[:, c])

    for zz in range(4):
        right, left = ((1, 0), (2, 3), (3, 2), (0, 1))[zz]

        @pl.when(z == zz)
        def _():
            if right:
                sent(2, nwg.at[:, 0, pl.ds(0, right)])
                sent(4, nwd.at[pl.ds(0, 5 * right), 0])
            if left:
                sent(3, nwg.at[:, 0, pl.ds(0, left)])
                sent(5, nwd.at[pl.ds(0, 5 * left), 0])


def train(x, dy, *arrays):
    anyspace = pl.BlockSpec(memory_space=pl.ANY)
    sds = jax.ShapeDtypeStruct
    dma = pltpu.SemaphoreType.DMA
    vm = pltpu.VMEM
    outs = (
        vm((NG, 2, 4, 160, C), BF), vm((NG, 2, 2, 64, D), BF),
        vm((2, 80, FF), F32), vm((2, 80, FF), F32), vm((2, 320, D), F32),
        vm((2, 80, FF), F32), vm((2, 80, FF), F32), vm((2, 320, D), F32),
        sds((T, D), BF), sds((T, D), BF),
    )
    return pl.pallas_call(
        kernel,
        out_shape=outs,
        in_specs=[anyspace] * 11,
        out_specs=(pl.BlockSpec(memory_space=pltpu.VMEM),) * 8 + (anyspace,) * 2,
        scratch_shapes=[
            vm((T, D), BF), vm((D, T), BF), vm((T, D), BF), vm((D, T), BF), vm((T, D), F32),
            vm((T, C), BF), vm((T, 2 * C), BF), vm((WS, D, 2 * C), BF), vm((WS, C, D), BF),
            vm((OWN, 2, 4, 160, C), BF), vm((OWN, 2, 2, 64, D), BF),
            vm((RING, 4, 160, C), BF), vm((RING, 2, 64, D), BF), vm((RING, 160, C), BF), vm((RING // 2, 2, 64, D), BF),
            vm((KEEP, 80, 2 * C), BF), vm((KEEP, 2, 64, D), BF),
            dma((10,)), dma((WS, 6)), dma((6,)), dma((8,)), dma((RING, 6)), dma((2, 4, 2)), dma((OWN, 2)), dma((NG,)), dma((NG,)),
            dma((NG, 5)), dma((NG, 2, 2)), dma((NG, 4)), dma((NG, 2)), dma((2,)),
        ],
        compiler_params=pltpu.CompilerParams(
            collective_id=0, has_side_effects=True, vmem_limit_bytes=37500000),
        name="train",
    )(x, dy, *arrays)


def place(nwg, nwd, *refs):
    moments, (wg, wu, wd), outs, (sem_out, sem_mo) = refs[:6], refs[6:9], refs[9:15], refs[15:]

    def moment(j):
        return pltpu.make_async_copy(moments[j], outs[j], sem_mo.at[j])

    def store(g, act):
        layer, i = 1 - g // NL, g % NL
        f = strips_of(i)

        @pl.loop(0, 8)
        def _(b):
            rows = pl.ds(pl.multiple_of(80 * b, 80), 80)
            for q, out in enumerate((wg, wu)):
                for k in range(2):
                    src = nwg.at[g, b % 2, b // 2, pl.ds(80 * q, 80), pl.ds(S * k, S)]
                    getattr(pltpu.make_async_copy(src, out.at[layer, rows, pl.ds(f[k], S)], sem_out.at[0]), act)()

        for core in range(2):
            for k in range(2):
                dest, off = down_piece(i, core, k)
                rows = pl.ds(pl.multiple_of(640 * dest + 320 * core + off, 64), 64)
                getattr(pltpu.make_async_copy(nwd.at[g, core, k], wd.at[layer, rows], sem_out.at[1]), act)()

    for j in range(6):
        moment(j).start()

    @pl.loop(0, NG)
    def _(g):
        store(g, "start")

    for j in range(6):
        moment(j).wait()

    @pl.loop(0, NG)
    def _(g):
        store(g, "wait")


def finish(*arrays):
    anyspace = pl.BlockSpec(memory_space=pl.ANY)
    sds = jax.ShapeDtypeStruct
    dma = pltpu.SemaphoreType.DMA
    moments = [sds(one.shape, one.dtype) for one in arrays[2:]]
    return pl.pallas_call(
        place,
        out_shape=(sds((2, D, FF), BF), sds((2, D, FF), BF), sds((2, FF, D), BF), *moments),
        in_specs=[pl.BlockSpec(memory_space=pltpu.VMEM)] * 8,
        out_specs=(anyspace,) * 9,
        scratch_shapes=[
            dma((2,)), dma((6,)),
        ],
        compiler_params=pltpu.CompilerParams(vmem_limit_bytes=2000000),
        name="place",
    )(*(pltpu.with_memory_space_constraint(one, pltpu.VMEM) for one in arrays))


def solution(mesh):
    def step(x, dy, *arrays):
        return finish(*train(x[0], dy[0], *arrays)[:8])

    whole = P(None, None, None)
    rows = P(None, "dp", None)
    seq = P(("rep", "dp"), None, None)
    return jax.shard_map(
        step,
        mesh=mesh,
        in_specs=(seq, seq) + (whole,) * 3 + (rows,) * 6,
        out_specs=(P("rep", None, None),) * 3 + (P("rep", "dp", None),) * 6,
        check_vma=False,
    )
```
